32 devices in a mesh: groups: 2 (over x), rows: 16 (over z, y, core).
Axes of the slice: x: 2, y: 2, z: 4, core: 2. Of those that a mesh axis runs over, the one named last changes fastest.
Arguments:
- phase: float32 [512, 2048], P(('groups', 'rows')), parts along dimension 0, may hold values from -3.140625 to 3.140625
Outputs:
- filtered: float32 [2, 512, 2048], P(None, ('groups', 'rows')), parts along dimension 1
- profile: float32 [6, 16], P('groups'), parts along dimension 0
The draws below stay inside these ranges and needn't reach their ends.
There are 2 independent parts, one for each index of `groups`. The reference program is written for one: setup_inputs(seed, part) draws one part's arguments, and reference() takes and returns one part's arrays. A program takes and returns all parts, laid end to end along the dimension named above; each array names one. Nothing has to cross between parts.
All inputs are finite; a program needn't handle non-finite values.
Results may differ from the reference program's by a relative error of at most 0.00012.
Values sent between devices are 32-bit elements; how exact they have to be, the bound alone decides.
A program may use at most 64 MiB of HBM per device.

```python
import jax
import jax.numpy as jnp
from jax import lax

COLS = 2048
ITERS = 3
NR = 256


def setup_inputs(seed: int = 0, part: int = 0) -> dict:
    streams_of = jax.random.split(jax.random.key(seed), 2)
    part_splits = jax.random.split(jax.random.fold_in(streams_of[1], part), 2)
    phase = jnp.clip(jax.random.uniform(part_splits[0], (NR, COLS), jnp.float32, -3.140625, 3.140625), -3.140625, 3.140625)
    return {"phase": phase}


EPS = 1e-6


def residue_sums(padded_rows):
    padded = jnp.pad(padded_rows, ((0, 0), (0, 0), (0, 1)))
    first = padded[:, :-1, :-1]
    second = padded[:, :-1, 1:]
    third = padded[:, 1:, 1:]
    fourth = padded[:, 1:, :-1]

    def cross(left, right):
        return left[1] * right[0] - left[0] * right[1]

    loop = cross(first, second) + cross(second, third) + cross(third, fourth) + cross(fourth, first)
    height = loop.shape[0]
    return jnp.sum((loop * loop).reshape(height, COLS // 128, 128), axis=(0, 2))


def goldstein(field, taper):
    extended = jnp.pad(field, ((0, 0), (0, 16), (0, 16)))
    blocks = extended.reshape(2, NR // 16 + 1, 16, COLS // 16 + 1, 16)

    def one_row(start):
        strip = lax.dynamic_slice_in_dim(blocks, start, 2, 1).reshape(2, 32, COLS // 16 + 1, 16)
        windows = jnp.concatenate([strip[:, :, :-1], strip[:, :, 1:]], axis=3)
        signal = windows[0] + 1j * windows[1]
        spectrum = jnp.fft.fft2(signal, axes=(0, 2))
        power = spectrum.real ** 2 + spectrum.imag ** 2
        average = jnp.mean(power, axis=(0, 2), keepdims=True)
        result = jnp.fft.ifft2(spectrum * (power / (average + EPS)) ** 0.25, axes=(0, 2)) * taper
        return jnp.stack([result.real, result.imag])

    pieces = lax.map(one_row, jnp.arange(NR // 16, dtype=jnp.int32))
    righty = jnp.pad(pieces[..., 16:], ((0, 0), (0, 0), (0, 0), (1, 0), (0, 0)))[:, :, :, :-1]
    columns = (pieces[..., :16] + righty).reshape(NR // 16, 2, 32, COLS)
    lower = jnp.pad(columns[:, :, 16:], ((1, 0), (0, 0), (0, 0), (0, 0)))[:-1]
    joined = columns[:, :, :16] + lower
    return joined.transpose(1, 0, 2, 3).reshape(2, NR, COLS)


def reference(phase):
    field = jnp.stack([jnp.cos(phase), jnp.sin(phase)])
    offsets = jnp.arange(32, dtype=jnp.float32)
    ramp = 1.0 - jnp.abs(offsets - 15.5) / 16.0
    taper = ramp[:, None, None] * ramp[None, None, :]
    reports = []
    for step in range(ITERS):
        padded_rows = jnp.pad(field, ((0, 0), (0, 1), (0, 0)))
        reports.append(residue_sums(padded_rows) / (NR * 128.0))
        field = goldstein(field, taper)
    return field, jnp.stack(reports)
```

```python
import functools
import math

import jax
import jax.numpy as jnp
from jax import lax
from jax.experimental import pallas as pl
from jax.experimental.pallas import tpu as pltpu
from jax.sharding import PartitionSpec as P

ITERS = 3
HALF = 16
WIN = 32
EPS = 1e-06
SLABS = ITERS + 2
PITCH = HALF + 1
GROUP = 8 * PITCH
AREA = HALF * HALF
SKEW = 8


def rotated(value, cosine, sine):
    real, imag = value
    if sine == 0.0:
        return value
    if cosine == 0.0:
        return (imag, -real) if sine > 0 else (-imag, real)
    if abs(cosine - sine) < 1e-12:
        return ((real + imag) * cosine, (imag - real) * cosine)
    if abs(cosine + sine) < 1e-12:
        return ((real - imag) * cosine, (imag + real) * cosine)
    return (real * cosine + imag * sine, imag * cosine - real * sine)


def twiddle(power, size):
    power = power % size
    exact = {0: (1.0, 0.0), size // 4: (0.0, 1.0), size // 2: (-1.0, 0.0), 3 * size // 4: (0.0, -1.0)}
    if power in exact:
        return exact[power]
    angle = 2.0 * math.pi * power / size
    return math.cos(angle), math.sin(angle)


def plus(a, b):
    return (a[0] + b[0], a[1] + b[1])


def minus(a, b):
    return (a[0] - b[0], a[1] - b[1])


def fft(values):
    size = len(values)
    if size == 1:
        return values
    if size == 2:
        return [plus(values[0], values[1]), minus(values[0], values[1])]
    even = fft(values[0::2])
    first = fft(values[1::4])
    third = fft(values[3::4])
    quarter = size // 4
    result = [None] * size
    for k in range(quarter):
        p = rotated(first[k], *twiddle(k, size))
        q = rotated(third[k], *twiddle(3 * k, size))
        total = plus(p, q)
        gap = minus(p, q)
        result[k] = plus(even[k], total)
        result[k + 2 * quarter] = minus(even[k], total)
        base = even[k + quarter]
        result[k + quarter] = (base[0] + gap[1], base[1] - gap[0])
        result[k + 3 * quarter] = (base[0] - gap[1], base[1] + gap[0])
    return result


def inverse_fft(values):
    swapped = fft([(imag, real) for real, imag in values])
    return [(real, imag) for imag, real in swapped]


def ramp(offset):
    return 1.0 - abs(offset - (WIN - 1) / 2) / HALF


SIN = [0.999999995726543, -0.1666665798726027, 0.008333051039470773, -0.00019809078301890923, 2.6052402754334837e-06]
COS = [0.9999999533642212, -0.4999990525190427, 0.041663583530066516, -0.001385370173749607, 2.315398040033116e-05]


def polynomial(coefficients, x):
    total = coefficients[-1]
    for c in coefficients[-2::-1]:
        total = total * x + c
    return total


def cos_sin(x):
    u = x * 0.5
    u2 = u * u
    s = u * polynomial(SIN, u2)
    c = polynomial(COS, u2)
    return 1.0 - 2.0 * s * s, 2.0 * s * c


def turned(value, cosine, sine):
    real, imag = value
    imag, real = rotated((imag, real), cosine, sine)
    return real, imag


def swap_blocks(pieces):
    lane = lax.broadcasted_iota(jnp.int32, pieces[0].shape, 1)

    def pick(values):
        for bit in (1, 2, 4):
            chosen = (lane & bit) != 0
            values = [jnp.where(chosen, values[i ^ bit], values[i]) for i in range(8)]
        return values

    moved = pick(pieces)
    moved = [moved[0]] + [jnp.take_along_axis(moved[r], lane ^ r, axis=1) for r in range(1, 8)]
    return pick(moved)


def kernel(n, lanes, x_ref, out_ref, prof_ref, own, ph, z, spec, cols, ahead_a, ahead_b, near_a, near_b,
           far_a, far_b, mine, heard, got, send_sem, recv_sem, give_sem, take_sem, tell_sem, hear_sem, known_sem):
    me = lax.axis_index("rows")
    side = 1 - 2 * lax.rem(me, 2)
    even = side == 1
    mesh = pl.DeviceIdType.MESH

    def inside(index):
        return jnp.logical_and(index >= 0, index < n)

    barrier = pltpu.get_barrier_semaphore()
    close = [side, -side, 2 * side, -2 * side, -3 * side]
    for d in close:
        @pl.when(inside(me + d))
        def _(d=d):
            pl.semaphore_signal(barrier, inc=1, device_id={"rows": me + d}, device_id_type=mesh)

    lane = lax.broadcasted_iota(jnp.int32, (8, lanes), 1)
    sub = lax.broadcasted_iota(jnp.int32, (8, lanes), 0)

    def next_block(x):
        return jnp.where(lane == lanes - 1, 0.0, pltpu.roll(x, lanes - 1, 1))

    def last_block(x):
        return jnp.where(lane == 0, 0.0, pltpu.roll(x, 1, 1))

    own_slot = 2 + side
    pair_slot = 2 + 2 * side

    for th in range(2):
        rows = x_ref[8 * th:8 * th + 8, :]
        stack = jnp.concatenate([rows[:, 128 * c:128 * c + 128] for c in range(16)], axis=0).T
        for h in range(2):
            blocks = swap_blocks([stack[16 * b + 8 * h:16 * b + 8 * h + 8] for b in range(8)])
            for t in range(8):
                at = (8 * th + t) * HALF + 8 * h
                own[at:at + 8, :] = blocks[t]

    def enter(source, slot):
        @pl.loop(0, 4)
        def _(q):
            for i in range(8):
                at = pl.ds(pl.multiple_of(q * 64, 64) + 8 * i, 8)
                c, s = cos_sin(source[at, :])
                z[0, slot, 0, at, :] = c
                z[0, slot, 1, at, :] = s

    def clear(buffer, slot):
        for c in range(2):
            z[buffer, slot, c, 0:AREA] = jnp.zeros((AREA, lanes), jnp.float32)

    count = 0
    for d in close:
        count = count + inside(me + d).astype(jnp.int32)
    pl.semaphore_wait(barrier, count)

    def phase_copy(d, slot, index):
        return pltpu.make_async_remote_copy(
            src_ref=own, dst_ref=ph.at[slot], send_sem=send_sem.at[index], recv_sem=recv_sem.at[slot],
            device_id={"rows": me + d}, device_id_type=mesh,
        )

    outgoing = [(side, 2 - 2 * side), (-side, 2), (2 * side, 2 - side), (-3 * side, 2 + 2 * side)]
    for index, (d, slot) in enumerate(outgoing):
        @pl.when(inside(me + d))
        def _(d=d, slot=slot, index=index):
            phase_copy(d, slot, index).start()

    reach = 2
    rounds = []
    while reach < n - 1:
        rounds.append(reach)
        reach *= 2

    def announce(i):
        for d in (-rounds[i], rounds[i]):
            @pl.when(inside(me + d))
            def _(d=d):
                pl.semaphore_signal(known_sem.at[i], inc=1, device_id={"rows": me + d}, device_id_type=mesh)

    def confirm(i):
        total = inside(me - rounds[i]).astype(jnp.int32) + inside(me + rounds[i]).astype(jnp.int32)
        pl.semaphore_wait(known_sem.at[i], total)

    def advance(i, last=False):
        if i > 0 and i <= len(rounds):
            confirm(i - 1)
        if i < len(rounds):
            announce(i)
        if last:
            for j in range(i + 1, len(rounds) + 1):
                advance(j)

    def arrive(slot, away):
        source = me + away
        valid = inside(source)

        @pl.when(valid)
        def _():
            pltpu.make_async_remote_copy(
                src_ref=own, dst_ref=ph.at[slot], send_sem=send_sem.at[0], recv_sem=recv_sem.at[slot],
                device_id={"rows": source}, device_id_type=mesh,
            ).wait_recv()
            enter(ph.at[slot], slot)

        @pl.when(jnp.logical_not(valid))
        def _():
            clear(0, slot)

    def profile(buffer, step):
        def row(slot, t):
            halves = []
            for c in range(2):
                base = t * HALF
                low = z[buffer, slot, c, pl.ds(base, 8), :]
                high = z[buffer, slot, c, pl.ds(base + 8, 8), :]
                low_next = z[buffer, slot, c, pl.ds(base + 1, 8), :]
                high_next = jnp.where(sub == 7, next_block(low)[0:1], z[buffer, slot, c, pl.ds(base + 9, 8), :])
                halves.append(((low, low_next), (high, high_next)))
            real, imag = halves
            return [(real[h][0], imag[h][0], real[h][1], imag[h][1]) for h in range(2)]

        def add(upper, lower, total):
            for u, v in zip(upper, lower):
                pr, pi = u[0] - v[2], u[1] - v[3]
                qr, qi = u[2] - v[0], u[3] - v[1]
                loop = pi * qr - pr * qi
                total = total + loop * loop
            return total

        def four(q, total):
            rows = [row(own_slot, 5 * q + t) for t in range(6)]
            for t in range(5):
                total = add(rows[t], rows[t + 1], total)
            return total

        total = lax.fori_loop(0, 3, four, jnp.zeros((8, lanes), jnp.float32))
        total = add(row(own_slot, HALF - 1), row(own_slot + 1, 0), total)
        mine[step:step + 1, :] = jnp.sum(total, axis=0, keepdims=True)

    aheads, nears, fars = (ahead_a, ahead_b), (near_a, near_b), (far_a, far_b)

    def window_row(buffer, upper, part):
        size = WIN if part is None else HALF
        groups = size // 8

        def ahead(g, ss):
            for s in ss:
                at = pl.ds(g * GROUP + s, 8, stride=PITCH)
                for c in range(2):
                    aheads[g % 2][c, 8 * s:8 * s + 8, :] = next_block(spec[c, at, :])

        def behind(g, ss):
            for s in ss:
                at = pl.ds(g * GROUP + s, 8, stride=PITCH)
                for c in range(2):
                    here = pl.ds(8 * s, 8)
                    cols[c, at, :] = nears[g % 2][c, here, :] + last_block(fars[g % 2][c, here, :])

        energy = jnp.zeros((8, lanes), jnp.float32)
        for h in range(2):
            values = []
            for t in range(WIN):
                at = pl.ds((t % HALF) * HALF + 8 * h, 8)
                values.append((z[buffer, upper + t // HALF, 0, at, :], z[buffer, upper + t // HALF, 1, at, :]))
            for real, imag in values:
                energy = energy + (real * real + imag * imag)
            if part == 0:
                values = [plus(values[t], values[t + HALF]) for t in range(HALF)]
            if part == 1:
                values = [rotated(minus(values[t], values[t + HALF]), *twiddle(t, WIN)) for t in range(HALF)]
            for k, value in enumerate(fft(values)):
                for c in range(2):
                    spec[c, pl.ds(k * PITCH + 8 * h, 8), :] = value[c]
            ahead(0, range(8 * h, 8 * h + 8))
        energy = jnp.broadcast_to(jnp.sum(energy, axis=0, keepdims=True), (8, lanes))
        scale = 1.0 / (energy + next_block(energy) + EPS)

        for g in range(groups):
            if g + 1 < groups:
                ahead(g + 1, range(HALF))
            if g > 0:
                behind(g - 1, range(HALF))
            values = []
            for s in range(HALF):
                at = pl.ds(g * GROUP + s, 8, stride=PITCH)
                values.append((spec[0, at, :], spec[1, at, :]))
            for s in range(HALF):
                here = pl.ds(8 * s, 8)
                values.append((aheads[g % 2][0, here, :], aheads[g % 2][1, here, :]))
            shaped = []
            for real, imag in fft(values):
                ratio = jnp.maximum((real * real + imag * imag) * scale, 1e-37)
                gain = lax.rsqrt(lax.rsqrt(ratio))
                shaped.append((real * gain, imag * gain))
            back = inverse_fft(shaped)
            for s in range(HALF):
                here = pl.ds(8 * s, 8)
                for c in range(2):
                    nears[g % 2][c, here, :] = back[s][c] * (ramp(s) / (WIN * WIN))
                    fars[g % 2][c, here, :] = back[s + HALF][c] * (ramp(s + HALF) / (WIN * WIN))

        for h in range(2):
            behind(groups - 1, range(8 * h, 8 * h + 8))
            values = []
            for k in range(size):
                at = pl.ds(k * PITCH + 8 * h, 8)
                values.append((cols[0, at, :], cols[1, at, :]))
            result = inverse_fft(values)
            if part == 1:
                result = [turned(value, *twiddle(t, WIN)) for t, value in enumerate(result)]
            for t in range(WIN):
                at = pl.ds((t % HALF) * HALF + 8 * h, 8)
                value = result[t % size]
                weight = -ramp(t) if part == 1 and t >= HALF else ramp(t)
                for c in range(2):
                    if part is None:
                        z[1 - buffer, upper + t // HALF, c, at, :] += value[c] * weight
                    else:
                        z[1 - buffer, upper + t // HALF, c, at, :] = value[c] * weight

    def middle(buffer):
        for part in range(2):
            @pl.when(lax.rem(me, 2) == part)
            def _(part=part):
                window_row(buffer, 3 * (1 - part), part)

    def give(step, which):
        buffer = (step + 1) % 2
        slot = pair_slot if which == 0 else own_slot
        return pltpu.make_async_remote_copy(
            src_ref=z.at[buffer, slot, :, pl.ds(0, AREA)], dst_ref=got.at[step, which],
            send_sem=give_sem.at[step, which], recv_sem=take_sem.at[step, which],
            device_id={"rows": me + side}, device_id_type=mesh,
        )

    def outer(step, q):
        buffer = step % 2
        upper = 1 + lax.rem(me, 2) * (q - 1) + (1 - lax.rem(me, 2)) * (2 - q)
        start = me + lax.rem(me, 2) * (q - 1) - (1 - lax.rem(me, 2)) * q
        far_slot = 2 - side * (q - 1)

        @pl.when(inside(start))
        def _():
            clear(1 - buffer, far_slot)
            window_row(buffer, upper, None)

        @pl.when(start + 1 == n)
        def _():
            clear(1 - buffer, far_slot)

    def settle(step, which):
        slot = own_slot if which == 0 else pair_slot
        buffer = (step + 1) % 2
        give(step, which).wait_recv()
        give(step, 1 - which).wait_send()
        for c in range(2):
            z[buffer, slot, c, 0:AREA] = z[buffer, slot, c, 0:AREA] + got[step, which, c]

    def tell(d):
        other = lax.rem(me + d, n)
        return pltpu.make_async_remote_copy(
            src_ref=mine, dst_ref=heard.at[n - d], send_sem=tell_sem.at[d], recv_sem=hear_sem.at[n - d],
            device_id={"rows": other}, device_id_type=mesh,
        )

    mine[...] = jnp.zeros_like(mine)
    enter(own, own_slot)
    advance(0)
    arrive(pair_slot, side)
    middle(0)
    give(0, 0).start()
    advance(1)

    @pl.loop(1, ITERS + 1)
    def _(q):
        arrive(2 - side * (q - 1), -side * q)
        outer(0, q)

        @pl.when(q == 1)
        def _():
            give(0, 1).start()
            profile(0, 0)

    for step in range(1, ITERS):
        settle(step - 1, 0)
        settle(step - 1, 1)
        profile(step % 2, step)
        if step == ITERS - 1:
            advance(3, last=True)

            @pl.loop(1, n)
            def _(d):
                tell(d).start()
        middle(step % 2)
        give(step, 0).start()
        if step < ITERS - 1:
            advance(2)

        @pl.loop(1, ITERS + 1 - step)
        def _(q, step=step):
            outer(step, q)
            if step < ITERS - 1:
                @pl.when(q == 1)
                def _():
                    give(step, 1).start()

    last = ITERS - 1
    give(last, 0).wait_recv()
    for c in range(2):
        for th in range(2):
            stack = [[None] * 2 for _ in range(8)]
            for h in range(2):
                pieces = []
                for t in range(8):
                    at = (8 * th + t) * HALF + 8 * h
                    pieces.append(z[ITERS % 2, own_slot, c, at:at + 8, :] + got[last, 0, c, at:at + 8, :])
                for b, block in enumerate(swap_blocks(pieces)):
                    stack[b][h] = block
            flat = jnp.concatenate([stack[b][h] for b in range(8) for h in range(2)], axis=0).T
            for k in range(16):
                out_ref[c, 8 * th:8 * th + 8, 128 * k:128 * k + 128] = flat[8 * k:8 * k + 8]
    give(last, 0).wait_send()

    for index, (d, slot) in enumerate(outgoing):
        @pl.when(inside(me + d))
        def _(d=d, slot=slot, index=index):
            phase_copy(d, slot, index).wait_send()

    def listen(d, total):
        tell(d).wait_send()
        pltpu.make_async_remote_copy(
            src_ref=mine, dst_ref=heard.at[d], send_sem=tell_sem.at[d], recv_sem=hear_sem.at[d],
            device_id={"rows": lax.rem(me + d, n)}, device_id_type=mesh,
        ).wait_recv()
        return total + heard[d]

    sums = lax.fori_loop(1, n, listen, mine[...])
    tiles = prof_ref.shape[1]
    per_tile = lanes // tiles
    rows = lax.broadcasted_iota(jnp.int32, (lanes, tiles), 0)
    low = lax.broadcasted_iota(jnp.int32, (lanes, tiles), 1) * per_tile
    member = jnp.where(jnp.logical_and(rows >= low, rows < low + per_tile), 1.0, 0.0)
    energy = jnp.dot(sums, member, precision=lax.Precision.HIGHEST, preferred_element_type=jnp.float32)
    prof_ref[...] = energy[:ITERS] / (HALF * n * 128.0)


def per_device(n, phase):
    slab, width = phase.shape
    assert slab == HALF and n % 2 == 0 and width == 128 * HALF
    lanes = width // HALF
    vmem = pltpu.VMEM
    f32 = jnp.float32
    return pl.pallas_call(
        functools.partial(kernel, n, lanes),
        out_shape=(
            jax.ShapeDtypeStruct((2, slab, width), f32),
            jax.ShapeDtypeStruct((ITERS, width // 128), f32),
        ),
        in_specs=[pl.BlockSpec(memory_space=vmem)],
        out_specs=(pl.BlockSpec(memory_space=vmem), pl.BlockSpec(memory_space=vmem)),
        scratch_shapes=[
            vmem((AREA, lanes), f32),
            vmem((SLABS, AREA, lanes), f32),
            vmem((2, SLABS, 2, AREA + SKEW, lanes), f32),
            vmem((2, WIN * PITCH + SKEW, lanes), f32),
            vmem((2, WIN * PITCH + SKEW, lanes), f32),
            *[vmem((2, 8 * HALF, lanes), f32) for _ in range(6)],
            vmem((8, lanes), f32),
            vmem((n, 8, lanes), f32),
            vmem((ITERS, 2, 2, AREA, lanes), f32),
            pltpu.SemaphoreType.DMA((4,)),
            pltpu.SemaphoreType.DMA((SLABS,)),
            pltpu.SemaphoreType.DMA((ITERS, 2)),
            pltpu.SemaphoreType.DMA((ITERS, 2)),
            pltpu.SemaphoreType.DMA((n,)),
            pltpu.SemaphoreType.DMA((n,)),
            pltpu.SemaphoreType.REGULAR((max(n.bit_length(), 1),)),
        ],
        compiler_params=pltpu.CompilerParams(collective_id=0, has_side_effects=True),
    )(phase)


def solution(mesh):
    return jax.shard_map(
        functools.partial(per_device, mesh.shape["rows"]),
        mesh=mesh,
        in_specs=(P(("groups", "rows"), None),),
        out_specs=(P(None, ("groups", "rows"), None), P("groups", None)),
        check_vma=False,
    )
```

```python
import functools
import math

import jax
import jax.numpy as jnp
from jax import lax
from jax.experimental import pallas as pl
from jax.experimental.pallas import tpu as pltpu
from jax.sharding import PartitionSpec as P

ITERS = 3
HALF = 16
WIN = 32
EPS = 1e-06
SLABS = ITERS + 2
PITCH = HALF + 1
GROUP = 8 * PITCH
AREA = HALF * HALF
SKEW = 8


def rotated(value, cosine, sine):
    real, imag = value
    if sine == 0.0:
        return value
    if cosine == 0.0:
        return (imag, -real) if sine > 0 else (-imag, real)
    if abs(cosine - sine) < 1e-12:
        return ((real + imag) * cosine, (imag - real) * cosine)
    if abs(cosine + sine) < 1e-12:
        return ((real - imag) * cosine, (imag + real) * cosine)
    return (real * cosine + imag * sine, imag * cosine - real * sine)


def twiddle(power, size):
    power = power % size
    exact = {0: (1.0, 0.0), size // 4: (0.0, 1.0), size // 2: (-1.0, 0.0), 3 * size // 4: (0.0, -1.0)}
    if power in exact:
        return exact[power]
    angle = 2.0 * math.pi * power / size
    return math.cos(angle), math.sin(angle)


def plus(a, b):
    return (a[0] + b[0], a[1] + b[1])


def minus(a, b):
    return (a[0] - b[0], a[1] - b[1])


def fft(values):
    size = len(values)
    if size == 1:
        return values
    if size == 2:
        return [plus(values[0], values[1]), minus(values[0], values[1])]
    even = fft(values[0::2])
    first = fft(values[1::4])
    third = fft(values[3::4])
    quarter = size // 4
    result = [None] * size
    for k in range(quarter):
        p = rotated(first[k], *twiddle(k, size))
        q = rotated(third[k], *twiddle(3 * k, size))
        total = plus(p, q)
        gap = minus(p, q)
        result[k] = plus(even[k], total)
        result[k + 2 * quarter] = minus(even[k], total)
        base = even[k + quarter]
        result[k + quarter] = (base[0] + gap[1], base[1] - gap[0])
        result[k + 3 * quarter] = (base[0] - gap[1], base[1] + gap[0])
    return result


def inverse_fft(values):
    swapped = fft([(imag, real) for real, imag in values])
    return [(real, imag) for imag, real in swapped]


def ramp(offset):
    return 1.0 - abs(offset - (WIN - 1) / 2) / HALF


SIN = [0.999999995726543, -0.1666665798726027, 0.008333051039470773, -0.00019809078301890923, 2.6052402754334837e-06]
COS = [0.9999999533642212, -0.4999990525190427, 0.041663583530066516, -0.001385370173749607, 2.315398040033116e-05]


def polynomial(coefficients, x):
    total = coefficients[-1]
    for c in coefficients[-2::-1]:
        total = total * x + c
    return total


def cos_sin(x):
    u = x * 0.5
    u2 = u * u
    s = u * polynomial(SIN, u2)
    c = polynomial(COS, u2)
    return 1.0 - 2.0 * s * s, 2.0 * s * c


def turned(value, cosine, sine):
    real, imag = value
    imag, real = rotated((imag, real), cosine, sine)
    return real, imag


def swap_blocks(pieces):
    lane = lax.broadcasted_iota(jnp.int32, pieces[0].shape, 1)

    def pick(values):
        for bit in (1, 2, 4):
            chosen = (lane & bit) != 0
            values = [jnp.where(chosen, values[i ^ bit], values[i]) for i in range(8)]
        return values

    moved = pick(pieces)
    moved = [moved[0]] + [jnp.take_along_axis(moved[r], lane ^ r, axis=1) for r in range(1, 8)]
    return pick(moved)


def kernel(n, lanes, x_ref, out_ref, prof_ref, own, ph, z, spec, cols, ahead_a, ahead_b, near_a, near_b,
           far_a, far_b, weights, mine, heard, got, send_sem, recv_sem, give_sem, take_sem, tell_sem, hear_sem, known_sem):
    me = lax.axis_index("rows")
    side = 1 - 2 * lax.rem(me, 2)
    even = side == 1
    mesh = pl.DeviceIdType.MESH

    def inside(index):
        return jnp.logical_and(index >= 0, index < n)

    barrier = pltpu.get_barrier_semaphore()
    close = [side, -side, 2 * side, -2 * side, -3 * side]
    for d in close:
        @pl.when(inside(me + d))
        def _(d=d):
            pl.semaphore_signal(barrier, inc=1, device_id={"rows": me + d}, device_id_type=mesh)

    lane = lax.broadcasted_iota(jnp.int32, (8, lanes), 1)
    sub = lax.broadcasted_iota(jnp.int32, (8, lanes), 0)

    def next_block(x):
        return jnp.where(lane == lanes - 1, 0.0, pltpu.roll(x, lanes - 1, 1))

    own_slot = 2 + side
    pair_slot = 2 + 2 * side

    for th in range(2):
        rows = x_ref[8 * th:8 * th + 8, :]
        stack = jnp.concatenate([rows[:, 128 * c:128 * c + 128] for c in range(16)], axis=0).T
        for h in range(2):
            blocks = swap_blocks([stack[16 * b + 8 * h:16 * b + 8 * h + 8] for b in range(8)])
            for t in range(8):
                at = (8 * th + t) * HALF + 8 * h
                own[at:at + 8, :] = blocks[t]

    def enter(source, slot):
        @pl.loop(0, 4)
        def _(q):
            for i in range(8):
                at = pl.ds(pl.multiple_of(q * 64, 64) + 8 * i, 8)
                c, s = cos_sin(source[at, :])
                z[0, slot, 0, at, :] = c
                z[0, slot, 1, at, :] = s

    def clear(buffer, slot):
        for c in range(2):
            z[buffer, slot, c, 0:AREA] = jnp.zeros((AREA, lanes), jnp.float32)

    count = 0
    for d in close:
        count = count + inside(me + d).astype(jnp.int32)
    pl.semaphore_wait(barrier, count)

    def phase_copy(d, slot, index):
        return pltpu.make_async_remote_copy(
            src_ref=own, dst_ref=ph.at[slot], send_sem=send_sem.at[index], recv_sem=recv_sem.at[slot],
            device_id={"rows": me + d}, device_id_type=mesh,
        )

    outgoing = [(side, 2 - 2 * side), (-side, 2), (2 * side, 2 - side), (-3 * side, 2 + 2 * side)]
    for index, (d, slot) in enumerate(outgoing):
        @pl.when(inside(me + d))
        def _(d=d, slot=slot, index=index):
            phase_copy(d, slot, index).start()

    reach = 2
    rounds = []
    while reach < n - 1:
        rounds.append(reach)
        reach *= 2

    def announce(i):
        for d in (-rounds[i], rounds[i]):
            @pl.when(inside(me + d))
            def _(d=d):
                pl.semaphore_signal(known_sem.at[i], inc=1, device_id={"rows": me + d}, device_id_type=mesh)

    def confirm(i):
        total = inside(me - rounds[i]).astype(jnp.int32) + inside(me + rounds[i]).astype(jnp.int32)
        pl.semaphore_wait(known_sem.at[i], total)

    def advance(i, last=False):
        if i > 0 and i <= len(rounds):
            confirm(i - 1)
        if i < len(rounds):
            announce(i)
        if last:
            for j in range(i + 1, len(rounds) + 1):
                advance(j)

    def arrive(slot, away):
        source = me + away
        valid = inside(source)

        @pl.when(valid)
        def _():
            pltpu.make_async_remote_copy(
                src_ref=own, dst_ref=ph.at[slot], send_sem=send_sem.at[0], recv_sem=recv_sem.at[slot],
                device_id={"rows": source}, device_id_type=mesh,
            ).wait_recv()
            enter(ph.at[slot], slot)

        @pl.when(jnp.logical_not(valid))
        def _():
            clear(0, slot)

    def profile(buffer, step):
        def row(slot, t):
            halves = []
            for c in range(2):
                base = t * HALF
                low = z[buffer, slot, c, pl.ds(base, 8), :]
                high = z[buffer, slot, c, pl.ds(base + 8, 8), :]
                low_next = z[buffer, slot, c, pl.ds(base + 1, 8), :]
                high_next = jnp.where(sub == 7, next_block(low)[0:1], z[buffer, slot, c, pl.ds(base + 9, 8), :])
                halves.append(((low, low_next), (high, high_next)))
            real, imag = halves
            return [(real[h][0], imag[h][0], real[h][1], imag[h][1]) for h in range(2)]

        def add(upper, lower, total):
            for u, v in zip(upper, lower):
                pr, pi = u[0] - v[2], u[1] - v[3]
                qr, qi = u[2] - v[0], u[3] - v[1]
                loop = pi * qr - pr * qi
                total = total + loop * loop
            return total

        def four(q, total):
            rows = [row(own_slot, 5 * q + t) for t in range(6)]
            for t in range(5):
                total = add(rows[t], rows[t + 1], total)
            return total

        total = lax.fori_loop(0, 3, four, jnp.zeros((8, lanes), jnp.float32))
        total = add(row(own_slot, HALF - 1), row(own_slot + 1, 0), total)
        mine[step:step + 1, :] = jnp.sum(total, axis=0, keepdims=True)

    aheads, nears, fars = (ahead_a, ahead_b), (near_a, near_b), (far_a, far_b)

    def window_row(buffer, upper, part):
        size = WIN if part is None else HALF
        groups = size // 8

        def ahead(g, ss):
            for s in ss:
                at = pl.ds(g * GROUP + s, 8, stride=PITCH)
                for c in range(2):
                    aheads[g % 2][c, 8 * s:8 * s + 8, :] = next_block(spec[c, at, :])

        def behind(g, ss):
            for s in ss:
                at = pl.ds(g * GROUP + s, 8, stride=PITCH)
                for c in range(2):
                    here = pl.ds(8 * s, 8)
                    cols[c, at, :] = nears[g % 2][c, here, :] + pltpu.roll(fars[g % 2][c, here, :], 1, 1)

        energy = jnp.zeros((8, lanes), jnp.float32)
        for h in range(2):
            values = []
            for t in range(WIN):
                at = pl.ds((t % HALF) * HALF + 8 * h, 8)
                values.append((z[buffer, upper + t // HALF, 0, at, :], z[buffer, upper + t // HALF, 1, at, :]))
            for real, imag in values:
                energy = energy + (real * real + imag * imag)
            if part == 0:
                values = [plus(values[t], values[t + HALF]) for t in range(HALF)]
            if part == 1:
                values = [rotated(minus(values[t], values[t + HALF]), *twiddle(t, WIN)) for t in range(HALF)]
            for k, value in enumerate(fft(values)):
                for c in range(2):
                    spec[c, pl.ds(k * PITCH + 8 * h, 8), :] = value[c]
            ahead(0, range(8 * h, 8 * h + 8))
        energy = jnp.broadcast_to(jnp.sum(energy, axis=0, keepdims=True), (8, lanes))
        energy = energy + next_block(energy) + EPS
        fourth = lax.rsqrt(energy * lax.rsqrt(energy)) / (WIN * WIN)
        kept = jnp.where(lane == lanes - 1, 0.0, fourth)
        for s in range(HALF):
            weights[0, 8 * s:8 * s + 8, :] = fourth * ramp(s)
            weights[1, 8 * s:8 * s + 8, :] = kept * ramp(s + HALF)

        for g in range(groups):
            if g + 1 < groups:
                ahead(g + 1, range(HALF))
            if g > 0:
                behind(g - 1, range(HALF))
            values = []
            for s in range(HALF):
                at = pl.ds(g * GROUP + s, 8, stride=PITCH)
                values.append((spec[0, at, :], spec[1, at, :]))
            for s in range(HALF):
                here = pl.ds(8 * s, 8)
                values.append((aheads[g % 2][0, here, :], aheads[g % 2][1, here, :]))
            shaped = []
            for real, imag in fft(values):
                gain = lax.rsqrt(lax.rsqrt(jnp.maximum(real * real + imag * imag, 1e-37)))
                shaped.append((real * gain, imag * gain))
            back = inverse_fft(shaped)
            for s in range(HALF):
                here = pl.ds(8 * s, 8)
                for c in range(2):
                    nears[g % 2][c, here, :] = back[s][c] * weights[0, here, :]
                    fars[g % 2][c, here, :] = back[s + HALF][c] * weights[1, here, :]

        for h in range(2):
            behind(groups - 1, range(8 * h, 8 * h + 8))
            values = []
            for k in range(size):
                at = pl.ds(k * PITCH + 8 * h, 8)
                values.append((cols[0, at, :], cols[1, at, :]))
            result = inverse_fft(values)
            if part == 1:
                result = [turned(value, *twiddle(t, WIN)) for t, value in enumerate(result)]
            for t in range(WIN):
                at = pl.ds((t % HALF) * HALF + 8 * h, 8)
                value = result[t % size]
                weight = -ramp(t) if part == 1 and t >= HALF else ramp(t)
                for c in range(2):
                    if part is None:
                        z[1 - buffer, upper + t // HALF, c, at, :] += value[c] * weight
                    else:
                        z[1 - buffer, upper + t // HALF, c, at, :] = value[c] * weight

    def middle(buffer):
        for part in range(2):
            @pl.when(lax.rem(me, 2) == part)
            def _(part=part):
                window_row(buffer, 3 * (1 - part), part)

    def give(step, which):
        buffer = (step + 1) % 2
        slot = pair_slot if which == 0 else own_slot
        return pltpu.make_async_remote_copy(
            src_ref=z.at[buffer, slot, :, pl.ds(0, AREA)], dst_ref=got.at[step, which],
            send_sem=give_sem.at[step, which], recv_sem=take_sem.at[step, which],
            device_id={"rows": me + side}, device_id_type=mesh,
        )

    def outer(buffer, q):
        upper = 1 + lax.rem(me, 2) * (q - 1) + (1 - lax.rem(me, 2)) * (2 - q)
        start = me + lax.rem(me, 2) * (q - 1) - (1 - lax.rem(me, 2)) * q
        far_slot = 2 - side * (q - 1)

        @pl.when(inside(start))
        def _():
            clear(1 - buffer, far_slot)
            window_row(buffer, upper, None)

        @pl.when(start + 1 == n)
        def _():
            clear(1 - buffer, far_slot)

    def settle(step, which):
        slot = own_slot if which == 0 else pair_slot
        buffer = (step + 1) % 2
        give(step, which).wait_recv()
        give(step, 1 - which).wait_send()
        for c in range(2):
            z[buffer, slot, c, 0:AREA] = z[buffer, slot, c, 0:AREA] + got[step, which, c]

    def tell(d):
        other = lax.rem(me + d, n)
        return pltpu.make_async_remote_copy(
            src_ref=mine, dst_ref=heard.at[n - d], send_sem=tell_sem.at[d], recv_sem=hear_sem.at[n - d],
            device_id={"rows": other}, device_id_type=mesh,
        )

    mine[...] = jnp.zeros_like(mine)
    enter(own, own_slot)
    advance(0)

    @pl.loop(0, 9)
    def _(i):
        def at(*turns):
            return functools.reduce(jnp.logical_or, [i == turn for turn in turns])

        def choose(table):
            return sum(jnp.where(i == turn, value, 0) for turn, value in table.items())

        central = at(0, 3, 7)
        step = choose({3: 1, 4: 1, 6: 1, 7: 2, 8: 2})
        q = choose({1: 1, 2: 2, 4: 1, 5: 3, 6: 2, 8: 1})
        buffer = lax.rem(step, 2)

        @pl.when(at(0, 1, 2, 5))
        def _():
            k = choose({0: -1, 1: 1, 2: 2, 5: 3})
            arrive(2 - side * (k - 1), -side * k)

        @pl.when(central)
        def _():
            middle(buffer)

        @pl.when(jnp.logical_not(central))
        def _():
            outer(buffer, q)

        @pl.when(i == 0)
        def _():
            give(0, 0).start()
            advance(1)

        @pl.when(i == 1)
        def _():
            give(0, 1).start()
            profile(0, 0)

        @pl.when(i == 2)
        def _():
            settle(0, 0)
            settle(0, 1)

        @pl.when(i == 3)
        def _():
            give(1, 0).start()

        @pl.when(i == 4)
        def _():
            give(1, 1).start()
            advance(2)
            profile(1, 1)

        @pl.when(i == 6)
        def _():
            settle(1, 0)
            settle(1, 1)
            profile(0, 2)
            advance(3, last=True)

            @pl.loop(1, n)
            def _(d):
                tell(d).start()

        @pl.when(i == 7)
        def _():
            give(2, 0).start()

    last = ITERS - 1
    give(last, 0).wait_recv()
    for c in range(2):
        for th in range(2):
            stack = [[None] * 2 for _ in range(8)]
            for h in range(2):
                pieces = []
                for t in range(8):
                    at = (8 * th + t) * HALF + 8 * h
                    pieces.append(z[ITERS % 2, own_slot, c, at:at + 8, :] + got[last, 0, c, at:at + 8, :])
                for b, block in enumerate(swap_blocks(pieces)):
                    stack[b][h] = block
            flat = jnp.concatenate([stack[b][h] for b in range(8) for h in range(2)], axis=0).T
            for k in range(16):
                out_ref[c, 8 * th:8 * th + 8, 128 * k:128 * k + 128] = flat[8 * k:8 * k + 8]
    give(last, 0).wait_send()

    for index, (d, slot) in enumerate(outgoing):
        @pl.when(inside(me + d))
        def _(d=d, slot=slot, index=index):
            phase_copy(d, slot, index).wait_send()

    def listen(d, total):
        tell(d).wait_send()
        pltpu.make_async_remote_copy(
            src_ref=mine, dst_ref=heard.at[d], send_sem=tell_sem.at[d], recv_sem=hear_sem.at[d],
            device_id={"rows": lax.rem(me + d, n)}, device_id_type=mesh,
        ).wait_recv()
        return total + heard[d]

    sums = lax.fori_loop(1, n, listen, mine[...])
    tiles = prof_ref.shape[1]
    per_tile = lanes // tiles
    rows = lax.broadcasted_iota(jnp.int32, (lanes, tiles), 0)
    low = lax.broadcasted_iota(jnp.int32, (lanes, tiles), 1) * per_tile
    member = jnp.where(jnp.logical_and(rows >= low, rows < low + per_tile), 1.0, 0.0)
    energy = jnp.dot(sums, member, precision=lax.Precision.HIGHEST, preferred_element_type=jnp.float32)
    prof_ref[...] = energy[:ITERS] / (HALF * n * 128.0)


def per_device(n, phase):
    slab, width = phase.shape
    assert ITERS == 3 and slab == HALF and n % 2 == 0 and width == 128 * HALF
    lanes = width // HALF
    vmem = pltpu.VMEM
    f32 = jnp.float32
    field, energy = pl.pallas_call(
        functools.partial(kernel, n, lanes),
        out_shape=(vmem((2, slab, width), f32), vmem((ITERS, width // 128), f32)),
        in_specs=[pl.BlockSpec(memory_space=vmem)],
        out_specs=(pl.BlockSpec(memory_space=vmem), pl.BlockSpec(memory_space=vmem)),
        scratch_shapes=[
            vmem((AREA, lanes), f32),
            vmem((SLABS, AREA, lanes), f32),
            vmem((2, SLABS, 2, AREA + SKEW, lanes), f32),
            vmem((2, WIN * PITCH + SKEW, lanes), f32),
            vmem((2, WIN * PITCH + SKEW, lanes), f32),
            *[vmem((2, 8 * HALF, lanes), f32) for _ in range(7)],
            vmem((8, lanes), f32),
            vmem((n, 8, lanes), f32),
            vmem((ITERS, 2, 2, AREA, lanes), f32),
            pltpu.SemaphoreType.DMA((4,)),
            pltpu.SemaphoreType.DMA((SLABS,)),
            pltpu.SemaphoreType.DMA((ITERS, 2)),
            pltpu.SemaphoreType.DMA((ITERS, 2)),
            pltpu.SemaphoreType.DMA((n,)),
            pltpu.SemaphoreType.DMA((n,)),
            pltpu.SemaphoreType.REGULAR((max(n.bit_length(), 1),)),
        ],
        compiler_params=pltpu.CompilerParams(collective_id=0, has_side_effects=True),
    )(phase)
    return pl.pallas_call(
        deliver,
        out_shape=(
            jax.ShapeDtypeStruct((2, slab, width), f32),
            jax.ShapeDtypeStruct((ITERS, width // 128), f32),
        ),
        in_specs=[pl.BlockSpec(memory_space=vmem)] * 2,
        out_specs=(pl.BlockSpec(memory_space=pl.ANY), pl.BlockSpec(memory_space=pl.ANY)),
        scratch_shapes=[pltpu.SemaphoreType.DMA((2,))],
    )(pltpu.with_memory_space_constraint(field, vmem), pltpu.with_memory_space_constraint(energy, vmem))


def deliver(field, energy, field_out, energy_out, sem):
    copies = [pltpu.make_async_copy(field, field_out, sem.at[0]), pltpu.make_async_copy(energy, energy_out, sem.at[1])]
    for copy in copies:
        copy.start()
    for copy in copies:
        copy.wait()


def solution(mesh):
    return jax.shard_map(
        functools.partial(per_device, mesh.shape["rows"]),
        mesh=mesh,
        in_specs=(P(("groups", "rows"), None),),
        out_specs=(P(None, ("groups", "rows"), None), P("groups", None)),
        check_vma=False,
    )
```

```python
import functools
import math

import jax
import jax.numpy as jnp
from jax import lax
from jax.experimental import pallas as pl
from jax.experimental.pallas import tpu as pltpu
from jax.sharding import PartitionSpec as P

ITERS = 3
HALF = 16
WIN = 32
EPS = 1e-06
SLABS = ITERS + 2
PITCH = HALF + 1
GROUP = 8 * PITCH
AREA = HALF * HALF
SKEW = 8


def rotated(value, cosine, sine):
    real, imag = value
    if sine == 0.0:
        return value
    if cosine == 0.0:
        return (imag, -real) if sine > 0 else (-imag, real)
    if abs(cosine - sine) < 1e-12:
        return ((real + imag) * cosine, (imag - real) * cosine)
    if abs(cosine + sine) < 1e-12:
        return ((real - imag) * cosine, (imag + real) * cosine)
    return (real * cosine + imag * sine, imag * cosine - real * sine)


def twiddle(power, size):
    power = power % size
    exact = {0: (1.0, 0.0), size // 4: (0.0, 1.0), size // 2: (-1.0, 0.0), 3 * size // 4: (0.0, -1.0)}
    if power in exact:
        return exact[power]
    angle = 2.0 * math.pi * power / size
    return math.cos(angle), math.sin(angle)


def plus(a, b):
    return (a[0] + b[0], a[1] + b[1])


def minus(a, b):
    return (a[0] - b[0], a[1] - b[1])


def fft(values):
    size = len(values)
    if size == 1:
        return values
    if size == 2:
        return [plus(values[0], values[1]), minus(values[0], values[1])]
    even = fft(values[0::2])
    first = fft(values[1::4])
    third = fft(values[3::4])
    quarter = size // 4
    result = [None] * size
    for k in range(quarter):
        p = rotated(first[k], *twiddle(k, size))
        q = rotated(third[k], *twiddle(3 * k, size))
        total = plus(p, q)
        gap = minus(p, q)
        result[k] = plus(even[k], total)
        result[k + 2 * quarter] = minus(even[k], total)
        base = even[k + quarter]
        result[k + quarter] = (base[0] + gap[1], base[1] - gap[0])
        result[k + 3 * quarter] = (base[0] - gap[1], base[1] + gap[0])
    return result


def inverse_fft(values):
    swapped = fft([(imag, real) for real, imag in values])
    return [(real, imag) for imag, real in swapped]


def ramp(offset):
    return 1.0 - abs(offset - (WIN - 1) / 2) / HALF


SIN = [0.999999995726543, -0.1666665798726027, 0.008333051039470773, -0.00019809078301890923, 2.6052402754334837e-06]
COS = [0.9999999533642212, -0.4999990525190427, 0.041663583530066516, -0.001385370173749607, 2.315398040033116e-05]


def polynomial(coefficients, x):
    total = coefficients[-1]
    for c in coefficients[-2::-1]:
        total = total * x + c
    return total


def cos_sin(x):
    u = x * 0.5
    u2 = u * u
    s = u * polynomial(SIN, u2)
    c = polynomial(COS, u2)
    return 1.0 - 2.0 * s * s, 2.0 * s * c


def turned(value, cosine, sine):
    real, imag = value
    imag, real = rotated((imag, real), cosine, sine)
    return real, imag


def swap_blocks(pieces):
    lane = lax.broadcasted_iota(jnp.int32, pieces[0].shape, 1)

    def pick(values):
        for bit in (1, 2, 4):
            chosen = (lane & bit) != 0
            values = [jnp.where(chosen, values[i ^ bit], values[i]) for i in range(8)]
        return values

    moved = pick(pieces)
    moved = [moved[0]] + [jnp.take_along_axis(moved[r], lane ^ r, axis=1) for r in range(1, 8)]
    return pick(moved)


def kernel(n, lanes, x_hbm, out_ref, prof_ref, x_ref, x_sem, own, ph, z, spec, cols, ahead_a, ahead_b, near_a, near_b,
           far_a, far_b, weights, mine, heard, got, send_sem, recv_sem, give_sem, take_sem, tell_sem, hear_sem, known_sem):
    me = lax.axis_index("rows")
    side = 1 - 2 * lax.rem(me, 2)
    even = side == 1
    mesh = pl.DeviceIdType.MESH

    def inside(index):
        return jnp.logical_and(index >= 0, index < n)

    barrier = pltpu.get_barrier_semaphore()
    close = [side, -side, 2 * side, -2 * side, -3 * side]
    for d in close:
        @pl.when(inside(me + d))
        def _(d=d):
            pl.semaphore_signal(barrier, inc=1, device_id={"rows": me + d}, device_id_type=mesh)

    fetch = pltpu.make_async_copy(x_hbm, x_ref, x_sem)
    fetch.start()

    lane = lax.broadcasted_iota(jnp.int32, (8, lanes), 1)
    sub = lax.broadcasted_iota(jnp.int32, (8, lanes), 0)

    def next_block(x):
        return jnp.where(lane == lanes - 1, 0.0, pltpu.roll(x, lanes - 1, 1))

    own_slot = 2 + side
    pair_slot = 2 + 2 * side

    fetch.wait()
    for th in range(2):
        rows = x_ref[8 * th:8 * th + 8, :]
        stack = jnp.concatenate([rows[:, 128 * c:128 * c + 128] for c in range(16)], axis=0).T
        for h in range(2):
            blocks = swap_blocks([stack[16 * b + 8 * h:16 * b + 8 * h + 8] for b in range(8)])
            for t in range(8):
                at = (8 * th + t) * HALF + 8 * h
                own[at:at + 8, :] = blocks[t]

    def enter(source, slot):
        @pl.loop(0, 4)
        def _(q):
            for i in range(8):
                at = pl.ds(pl.multiple_of(q * 64, 64) + 8 * i, 8)
                c, s = cos_sin(source[at, :])
                z[0, slot, 0, at, :] = c
                z[0, slot, 1, at, :] = s

    def clear(buffer, slot):
        for c in range(2):
            z[buffer, slot, c, 0:AREA] = jnp.zeros((AREA, lanes), jnp.float32)

    count = 0
    for d in close:
        count = count + inside(me + d).astype(jnp.int32)
    pl.semaphore_wait(barrier, count)

    def phase_copy(d, slot, index):
        return pltpu.make_async_remote_copy(
            src_ref=own, dst_ref=ph.at[slot], send_sem=send_sem.at[index], recv_sem=recv_sem.at[slot],
            device_id={"rows": me + d}, device_id_type=mesh,
        )

    outgoing = [(side, 2 - 2 * side), (-side, 2), (2 * side, 2 - side), (-3 * side, 2 + 2 * side)]
    for index, (d, slot) in enumerate(outgoing):
        @pl.when(inside(me + d))
        def _(d=d, slot=slot, index=index):
            phase_copy(d, slot, index).start()

    reach = 2
    rounds = []
    while reach < n - 1:
        rounds.append(reach)
        reach *= 2

    def announce(i):
        for d in (-rounds[i], rounds[i]):
            @pl.when(inside(me + d))
            def _(d=d):
                pl.semaphore_signal(known_sem.at[i], inc=1, device_id={"rows": me + d}, device_id_type=mesh)

    def confirm(i):
        total = inside(me - rounds[i]).astype(jnp.int32) + inside(me + rounds[i]).astype(jnp.int32)
        pl.semaphore_wait(known_sem.at[i], total)

    def advance(i, last=False):
        if i > 0 and i <= len(rounds):
            confirm(i - 1)
        if i < len(rounds):
            announce(i)
        if last:
            for j in range(i + 1, len(rounds) + 1):
                advance(j)

    def arrive(slot, away):
        source = me + away
        valid = inside(source)

        @pl.when(valid)
        def _():
            pltpu.make_async_remote_copy(
                src_ref=own, dst_ref=ph.at[slot], send_sem=send_sem.at[0], recv_sem=recv_sem.at[slot],
                device_id={"rows": source}, device_id_type=mesh,
            ).wait_recv()
            enter(ph.at[slot], slot)

        @pl.when(jnp.logical_not(valid))
        def _():
            clear(0, slot)

    def profile(buffer, step):
        def row(slot, t):
            halves = []
            for c in range(2):
                base = t * HALF
                low = z[buffer, slot, c, pl.ds(base, 8), :]
                high = z[buffer, slot, c, pl.ds(base + 8, 8), :]
                low_next = z[buffer, slot, c, pl.ds(base + 1, 8), :]
                high_next = jnp.where(sub == 7, next_block(low)[0:1], z[buffer, slot, c, pl.ds(base + 9, 8), :])
                halves.append(((low, low_next), (high, high_next)))
            real, imag = halves
            return [(real[h][0], imag[h][0], real[h][1], imag[h][1]) for h in range(2)]

        def add(upper, lower, total):
            for u, v in zip(upper, lower):
                pr, pi = u[0] - v[2], u[1] - v[3]
                qr, qi = u[2] - v[0], u[3] - v[1]
                loop = pi * qr - pr * qi
                total = total + loop * loop
            return total

        def four(q, total):
            rows = [row(own_slot, 5 * q + t) for t in range(6)]
            for t in range(5):
                total = add(rows[t], rows[t + 1], total)
            return total

        total = lax.fori_loop(0, 3, four, jnp.zeros((8, lanes), jnp.float32))
        total = add(row(own_slot, HALF - 1), row(own_slot + 1, 0), total)
        mine[step:step + 1, :] = jnp.sum(total, axis=0, keepdims=True)

    aheads, nears, fars = (ahead_a, ahead_b), (near_a, near_b), (far_a, far_b)

    def window_row(buffer, upper, part):
        size = WIN if part is None else HALF
        groups = size // 8

        def ahead(g, ss):
            for s in ss:
                at = pl.ds(g * GROUP + s, 8, stride=PITCH)
                for c in range(2):
                    aheads[g % 2][c, 8 * s:8 * s + 8, :] = next_block(spec[c, at, :])

        def behind(g, ss):
            for s in ss:
                at = pl.ds(g * GROUP + s, 8, stride=PITCH)
                for c in range(2):
                    here = pl.ds(8 * s, 8)
                    cols[c, at, :] = nears[g % 2][c, here, :] + pltpu.roll(fars[g % 2][c, here, :], 1, 1)

        energy = jnp.zeros((8, lanes), jnp.float32)
        for h in range(2):
            values = []
            for t in range(WIN):
                at = pl.ds((t % HALF) * HALF + 8 * h, 8)
                values.append((z[buffer, upper + t // HALF, 0, at, :], z[buffer, upper + t // HALF, 1, at, :]))
            for real, imag in values:
                energy = energy + (real * real + imag * imag)
            if part == 0:
                values = [plus(values[t], values[t + HALF]) for t in range(HALF)]
            if part == 1:
                values = [rotated(minus(values[t], values[t + HALF]), *twiddle(t, WIN)) for t in range(HALF)]
            for k, value in enumerate(fft(values)):
                for c in range(2):
                    spec[c, pl.ds(k * PITCH + 8 * h, 8), :] = value[c]
            ahead(0, range(8 * h, 8 * h + 8))
        energy = jnp.broadcast_to(jnp.sum(energy, axis=0, keepdims=True), (8, lanes))
        energy = energy + next_block(energy) + EPS
        fourth = lax.rsqrt(energy * lax.rsqrt(energy)) / (WIN * WIN)
        kept = jnp.where(lane == lanes - 1, 0.0, fourth)
        for s in range(HALF):
            weights[0, 8 * s:8 * s + 8, :] = fourth * ramp(s)
            weights[1, 8 * s:8 * s + 8, :] = kept * ramp(s + HALF)

        for g in range(groups):
            if g + 1 < groups:
                ahead(g + 1, range(HALF))
            if g > 0:
                behind(g - 1, range(HALF))
            values = []
            for s in range(HALF):
                at = pl.ds(g * GROUP + s, 8, stride=PITCH)
                values.append((spec[0, at, :], spec[1, at, :]))
            for s in range(HALF):
                here = pl.ds(8 * s, 8)
                values.append((aheads[g % 2][0, here, :], aheads[g % 2][1, here, :]))
            shaped = []
            for real, imag in fft(values):
                gain = lax.rsqrt(lax.rsqrt(jnp.maximum(real * real + imag * imag, 1e-37)))
                shaped.append((real * gain, imag * gain))
            back = inverse_fft(shaped)
            for s in range(HALF):
                here = pl.ds(8 * s, 8)
                for c in range(2):
                    nears[g % 2][c, here, :] = back[s][c] * weights[0, here, :]
                    fars[g % 2][c, here, :] = back[s + HALF][c] * weights[1, here, :]

        for h in range(2):
            behind(groups - 1, range(8 * h, 8 * h + 8))
            values = []
            for k in range(size):
                at = pl.ds(k * PITCH + 8 * h, 8)
                values.append((cols[0, at, :], cols[1, at, :]))
            result = inverse_fft(values)
            if part == 1:
                result = [turned(value, *twiddle(t, WIN)) for t, value in enumerate(result)]
            for t in range(WIN):
                at = pl.ds((t % HALF) * HALF + 8 * h, 8)
                value = result[t % size]
                weight = -ramp(t) if part == 1 and t >= HALF else ramp(t)
                for c in range(2):
                    if part is None:
                        z[1 - buffer, upper + t // HALF, c, at, :] += value[c] * weight
                    else:
                        z[1 - buffer, upper + t // HALF, c, at, :] = value[c] * weight

    def middle(buffer):
        for part in range(2):
            @pl.when(lax.rem(me, 2) == part)
            def _(part=part):
                window_row(buffer, 3 * (1 - part), part)

    def give(step, which):
        buffer = (step + 1) % 2
        slot = pair_slot if which == 0 else own_slot
        return pltpu.make_async_remote_copy(
            src_ref=z.at[buffer, slot, :, pl.ds(0, AREA)], dst_ref=got.at[step, which],
            send_sem=give_sem.at[step, which], recv_sem=take_sem.at[step, which],
            device_id={"rows": me + side}, device_id_type=mesh,
        )

    def outer(buffer, q):
        upper = 1 + lax.rem(me, 2) * (q - 1) + (1 - lax.rem(me, 2)) * (2 - q)
        start = me + lax.rem(me, 2) * (q - 1) - (1 - lax.rem(me, 2)) * q
        far_slot = 2 - side * (q - 1)

        @pl.when(inside(start))
        def _():
            clear(1 - buffer, far_slot)
            window_row(buffer, upper, None)

        @pl.when(start + 1 == n)
        def _():
            clear(1 - buffer, far_slot)

    def settle(step, which):
        slot = own_slot if which == 0 else pair_slot
        buffer = (step + 1) % 2
        give(step, which).wait_recv()
        give(step, 1 - which).wait_send()
        for c in range(2):
            z[buffer, slot, c, 0:AREA] = z[buffer, slot, c, 0:AREA] + got[step, which, c]

    def tell(d):
        other = lax.rem(me + d, n)
        return pltpu.make_async_remote_copy(
            src_ref=mine.at[pl.ds(0, ITERS)], dst_ref=heard.at[n - d, pl.ds(0, ITERS)], send_sem=tell_sem.at[d], recv_sem=hear_sem.at[n - d],
            device_id={"rows": other}, device_id_type=mesh,
        )

    mine[...] = jnp.zeros_like(mine)
    enter(own, own_slot)
    advance(0)

    @pl.loop(0, 9)
    def _(i):
        def at(*turns):
            return functools.reduce(jnp.logical_or, [i == turn for turn in turns])

        def choose(table):
            return sum(jnp.where(i == turn, value, 0) for turn, value in table.items())

        central = at(0, 3, 7)
        step = choose({3: 1, 4: 1, 6: 1, 7: 2, 8: 2})
        q = choose({1: 1, 2: 2, 4: 1, 5: 3, 6: 2, 8: 1})
        buffer = lax.rem(step, 2)

        @pl.when(at(0, 1, 2, 5))
        def _():
            k = choose({0: -1, 1: 1, 2: 2, 5: 3})
            arrive(2 - side * (k - 1), -side * k)

        @pl.when(central)
        def _():
            middle(buffer)

        @pl.when(jnp.logical_not(central))
        def _():
            outer(buffer, q)

        @pl.when(i == 0)
        def _():
            give(0, 0).start()
            advance(1)

        @pl.when(i == 1)
        def _():
            give(0, 1).start()
            profile(0, 0)

        @pl.when(i == 2)
        def _():
            settle(0, 0)
            settle(0, 1)

        @pl.when(i == 3)
        def _():
            give(1, 0).start()

        @pl.when(i == 4)
        def _():
            give(1, 1).start()
            advance(2)
            profile(1, 1)

        @pl.when(i == 6)
        def _():
            settle(1, 0)
            settle(1, 1)
            profile(0, 2)
            advance(3, last=True)

            @pl.loop(1, n)
            def _(d):
                tell(d).start()

        @pl.when(i == 7)
        def _():
            give(2, 0).start()

    last = ITERS - 1
    give(last, 0).wait_recv()
    for c in range(2):
        for th in range(2):
            stack = [[None] * 2 for _ in range(8)]
            for h in range(2):
                pieces = []
                for t in range(8):
                    at = (8 * th + t) * HALF + 8 * h
                    pieces.append(z[ITERS % 2, own_slot, c, at:at + 8, :] + got[last, 0, c, at:at + 8, :])
                for b, block in enumerate(swap_blocks(pieces)):
                    stack[b][h] = block
            flat = jnp.concatenate([stack[b][h] for b in range(8) for h in range(2)], axis=0).T
            for k in range(16):
                out_ref[c, 8 * th:8 * th + 8, 128 * k:128 * k + 128] = flat[8 * k:8 * k + 8]
    give(last, 0).wait_send()

    for index, (d, slot) in enumerate(outgoing):
        @pl.when(inside(me + d))
        def _(d=d, slot=slot, index=index):
            phase_copy(d, slot, index).wait_send()

    def listen(d, total):
        tell(d).wait_send()
        pltpu.make_async_remote_copy(
            src_ref=mine.at[pl.ds(0, ITERS)], dst_ref=heard.at[d, pl.ds(0, ITERS)], send_sem=tell_sem.at[d], recv_sem=hear_sem.at[d],
            device_id={"rows": lax.rem(me + d, n)}, device_id_type=mesh,
        ).wait_recv()
        return total + heard[d, 0:ITERS, :]

    sums = lax.fori_loop(1, n, listen, mine[0:ITERS, :])
    tiles = prof_ref.shape[1]
    per_tile = lanes // tiles
    rows = lax.broadcasted_iota(jnp.int32, (lanes, tiles), 0)
    low = lax.broadcasted_iota(jnp.int32, (lanes, tiles), 1) * per_tile
    member = jnp.where(jnp.logical_and(rows >= low, rows < low + per_tile), 1.0, 0.0)
    energy = jnp.dot(sums, member, precision=lax.Precision.HIGHEST, preferred_element_type=jnp.float32)
    prof_ref[...] = energy / (HALF * n * 128.0)


def per_device(n, phase):
    slab, width = phase.shape
    assert ITERS == 3 and slab == HALF and n % 2 == 0 and width == 128 * HALF
    lanes = width // HALF
    vmem = pltpu.VMEM
    f32 = jnp.float32
    field, energy = pl.pallas_call(
        functools.partial(kernel, n, lanes),
        out_shape=(vmem((2, slab, width), f32), vmem((ITERS, width // 128), f32)),
        in_specs=[pl.BlockSpec(memory_space=pl.ANY)],
        out_specs=(pl.BlockSpec(memory_space=vmem), pl.BlockSpec(memory_space=vmem)),
        scratch_shapes=[
            vmem((slab, width), f32),
            pltpu.SemaphoreType.DMA,
            vmem((AREA, lanes), f32),
            vmem((SLABS, AREA, lanes), f32),
            vmem((2, SLABS, 2, AREA + SKEW, lanes), f32),
            vmem((2, WIN * PITCH + SKEW, lanes), f32),
            vmem((2, WIN * PITCH + SKEW, lanes), f32),
            *[vmem((2, 8 * HALF, lanes), f32) for _ in range(7)],
            vmem((8, lanes), f32),
            vmem((n, 8, lanes), f32),
            vmem((ITERS, 2, 2, AREA, lanes), f32),
            pltpu.SemaphoreType.DMA((4,)),
            pltpu.SemaphoreType.DMA((SLABS,)),
            pltpu.SemaphoreType.DMA((ITERS, 2)),
            pltpu.SemaphoreType.DMA((ITERS, 2)),
            pltpu.SemaphoreType.DMA((n,)),
            pltpu.SemaphoreType.DMA((n,)),
            pltpu.SemaphoreType.REGULAR((max(n.bit_length(), 1),)),
        ],
        compiler_params=pltpu.CompilerParams(collective_id=0, has_side_effects=True),
    )(phase)
    return pl.pallas_call(
        deliver,
        out_shape=(
            jax.ShapeDtypeStruct((2, slab, width), f32),
            jax.ShapeDtypeStruct((ITERS, width // 128), f32),
        ),
        in_specs=[pl.BlockSpec(memory_space=vmem)] * 2,
        out_specs=(pl.BlockSpec(memory_space=pl.ANY), pl.BlockSpec(memory_space=pl.ANY)),
        scratch_shapes=[pltpu.SemaphoreType.DMA((2,))],
    )(pltpu.with_memory_space_constraint(field, vmem), pltpu.with_memory_space_constraint(energy, vmem))


def deliver(field, energy, field_out, energy_out, sem):
    copies = [pltpu.make_async_copy(field, field_out, sem.at[0]), pltpu.make_async_copy(energy, energy_out, sem.at[1])]
    for copy in copies:
        copy.start()
    for copy in copies:
        copy.wait()


def solution(mesh):
    return jax.shard_map(
        functools.partial(per_device, mesh.shape["rows"]),
        mesh=mesh,
        in_specs=(P(("groups", "rows"), None),),
        out_specs=(P(None, ("groups", "rows"), None), P("groups", None)),
        check_vma=False,
    )
```

```python
import functools
import math

import jax
import jax.numpy as jnp
from jax import lax
from jax.experimental import pallas as pl
from jax.experimental.pallas import tpu as pltpu
from jax.sharding import PartitionSpec as P

ITERS = 3
HALF = 16
WIN = 32
EPS = 1e-06
SLABS = ITERS + 2
PITCH = HALF + 1
GROUP = 8 * PITCH
AREA = HALF * HALF
SKEW = 8


def rotated(value, cosine, sine):
    real, imag = value
    if sine == 0.0:
        return value
    if cosine == 0.0:
        return (imag, -real) if sine > 0 else (-imag, real)
    if abs(cosine - sine) < 1e-12:
        return ((real + imag) * cosine, (imag - real) * cosine)
    if abs(cosine + sine) < 1e-12:
        return ((real - imag) * cosine, (imag + real) * cosine)
    return (real * cosine + imag * sine, imag * cosine - real * sine)


def twiddle(power, size):
    power = power % size
    exact = {0: (1.0, 0.0), size // 4: (0.0, 1.0), size // 2: (-1.0, 0.0), 3 * size // 4: (0.0, -1.0)}
    if power in exact:
        return exact[power]
    angle = 2.0 * math.pi * power / size
    return math.cos(angle), math.sin(angle)


def plus(a, b):
    return (a[0] + b[0], a[1] + b[1])


def minus(a, b):
    return (a[0] - b[0], a[1] - b[1])


def fft(values):
    size = len(values)
    if size == 1:
        return values
    if size == 2:
        return [plus(values[0], values[1]), minus(values[0], values[1])]
    even = fft(values[0::2])
    first = fft(values[1::4])
    third = fft(values[3::4])
    quarter = size // 4
    result = [None] * size
    for k in range(quarter):
        p = rotated(first[k], *twiddle(k, size))
        q = rotated(third[k], *twiddle(3 * k, size))
        total = plus(p, q)
        gap = minus(p, q)
        result[k] = plus(even[k], total)
        result[k + 2 * quarter] = minus(even[k], total)
        base = even[k + quarter]
        result[k + quarter] = (base[0] + gap[1], base[1] - gap[0])
        result[k + 3 * quarter] = (base[0] - gap[1], base[1] + gap[0])
    return result


def inverse_fft(values):
    swapped = fft([(imag, real) for real, imag in values])
    return [(real, imag) for imag, real in swapped]


def ramp(offset):
    return 1.0 - abs(offset - (WIN - 1) / 2) / HALF


SIN = [0.999999995726543, -0.1666665798726027, 0.008333051039470773, -0.00019809078301890923, 2.6052402754334837e-06]
COS = [0.9999999533642212, -0.4999990525190427, 0.041663583530066516, -0.001385370173749607, 2.315398040033116e-05]


def polynomial(coefficients, x):
    total = coefficients[-1]
    for c in coefficients[-2::-1]:
        total = total * x + c
    return total


def cos_sin(x):
    u = x * 0.5
    u2 = u * u
    s = u * polynomial(SIN, u2)
    c = polynomial(COS, u2)
    return 1.0 - 2.0 * s * s, 2.0 * s * c


def turned(value, cosine, sine):
    real, imag = value
    imag, real = rotated((imag, real), cosine, sine)
    return real, imag


def swap_blocks(pieces):
    lane = lax.broadcasted_iota(jnp.int32, pieces[0].shape, 1)

    def pick(values):
        for bit in (1, 2, 4):
            chosen = (lane & bit) != 0
            values = [jnp.where(chosen, values[i ^ bit], values[i]) for i in range(8)]
        return values

    moved = pick(pieces)
    moved = [moved[0]] + [jnp.take_along_axis(moved[r], lane ^ r, axis=1) for r in range(1, 8)]
    return pick(moved)


def kernel(n, lanes, x_hbm, out_ref, prof_ref, x_ref, x_sem, own, ph, z, spec, cols, ahead_a, ahead_b, near_a, near_b,
           far_a, far_b, weights, mine, heard, got, send_sem, recv_sem, give_sem, take_sem, tell_sem, hear_sem, known_sem):
    me = lax.axis_index("rows")
    side = 1 - 2 * lax.rem(me, 2)
    even = side == 1
    mesh = pl.DeviceIdType.MESH

    def inside(index):
        return jnp.logical_and(index >= 0, index < n)

    barrier = pltpu.get_barrier_semaphore()
    close = [side, -side, 2 * side, -2 * side, -3 * side]
    for d in close:
        @pl.when(inside(me + d))
        def _(d=d):
            pl.semaphore_signal(barrier, inc=1, device_id={"rows": me + d}, device_id_type=mesh)

    fetch = pltpu.make_async_copy(x_hbm, x_ref, x_sem)
    fetch.start()

    lane = lax.broadcasted_iota(jnp.int32, (8, lanes), 1)
    sub = lax.broadcasted_iota(jnp.int32, (8, lanes), 0)

    def next_block(x):
        return jnp.where(lane == lanes - 1, 0.0, pltpu.roll(x, lanes - 1, 1))

    own_slot = 2 + side
    pair_slot = 2 + 2 * side

    fetch.wait()
    for th in range(2):
        rows = x_ref[8 * th:8 * th + 8, :]
        stack = jnp.concatenate([rows[:, 128 * c:128 * c + 128] for c in range(16)], axis=0).T
        for h in range(2):
            blocks = swap_blocks([stack[16 * b + 8 * h:16 * b + 8 * h + 8] for b in range(8)])
            for t in range(8):
                at = (8 * th + t) * HALF + 8 * h
                own[at:at + 8, :] = blocks[t]

    def enter(source, slot):
        @pl.loop(0, 4)
        def _(q):
            for i in range(8):
                at = pl.ds(pl.multiple_of(q * 64, 64) + 8 * i, 8)
                c, s = cos_sin(source[at, :])
                z[0, slot, 0, at, :] = c
                z[0, slot, 1, at, :] = s

    def clear(buffer, slot):
        for c in range(2):
            z[buffer, slot, c, 0:AREA] = jnp.zeros((AREA, lanes), jnp.float32)

    count = 0
    for d in close:
        count = count + inside(me + d).astype(jnp.int32)
    pl.semaphore_wait(barrier, count)

    def phase_copy(d, slot, index):
        return pltpu.make_async_remote_copy(
            src_ref=own, dst_ref=ph.at[slot], send_sem=send_sem.at[index], recv_sem=recv_sem.at[slot],
            device_id={"rows": me + d}, device_id_type=mesh,
        )

    outgoing = [(side, 2 - 2 * side), (-side, 2), (2 * side, 2 - side), (-3 * side, 2 + 2 * side)]
    for index, (d, slot) in enumerate(outgoing):
        @pl.when(inside(me + d))
        def _(d=d, slot=slot, index=index):
            phase_copy(d, slot, index).start()

    reach = 2
    rounds = []
    while reach < n - 1:
        rounds.append(reach)
        reach *= 2

    def announce(i):
        for d in (-rounds[i], rounds[i]):
            @pl.when(inside(me + d))
            def _(d=d):
                pl.semaphore_signal(known_sem.at[i], inc=1, device_id={"rows": me + d}, device_id_type=mesh)

    def confirm(i):
        total = inside(me - rounds[i]).astype(jnp.int32) + inside(me + rounds[i]).astype(jnp.int32)
        pl.semaphore_wait(known_sem.at[i], total)

    def advance(i, last=False):
        if i > 0 and i <= len(rounds):
            confirm(i - 1)
        if i < len(rounds):
            announce(i)
        if last:
            for j in range(i + 1, len(rounds) + 1):
                advance(j)

    def arrive(slot, away):
        source = me + away
        valid = inside(source)

        @pl.when(valid)
        def _():
            pltpu.make_async_remote_copy(
                src_ref=own, dst_ref=ph.at[slot], send_sem=send_sem.at[0], recv_sem=recv_sem.at[slot],
                device_id={"rows": source}, device_id_type=mesh,
            ).wait_recv()
            enter(ph.at[slot], slot)

        @pl.when(jnp.logical_not(valid))
        def _():
            clear(0, slot)

    def profile(buffer, step):
        def row(slot, t):
            halves = []
            for c in range(2):
                base = t * HALF
                low = z[buffer, slot, c, pl.ds(base, 8), :]
                high = z[buffer, slot, c, pl.ds(base + 8, 8), :]
                low_next = z[buffer, slot, c, pl.ds(base + 1, 8), :]
                high_next = jnp.where(sub == 7, next_block(low)[0:1], z[buffer, slot, c, pl.ds(base + 9, 8), :])
                halves.append(((low, low_next), (high, high_next)))
            real, imag = halves
            return [(real[h][0], imag[h][0], real[h][1], imag[h][1]) for h in range(2)]

        def add(upper, lower, total):
            for u, v in zip(upper, lower):
                pr, pi = u[0] - v[2], u[1] - v[3]
                qr, qi = u[2] - v[0], u[3] - v[1]
                loop = pi * qr - pr * qi
                total = total + loop * loop
            return total

        def four(q, total):
            rows = [row(own_slot, 5 * q + t) for t in range(6)]
            for t in range(5):
                total = add(rows[t], rows[t + 1], total)
            return total

        total = lax.fori_loop(0, 3, four, jnp.zeros((8, lanes), jnp.float32))
        total = add(row(own_slot, HALF - 1), row(own_slot + 1, 0), total)
        mine[step:step + 1, :] = jnp.sum(total, axis=0, keepdims=True)

    aheads, nears, fars = (ahead_a, ahead_b), (near_a, near_b), (far_a, far_b)

    def window_row(buffer, upper, part):
        size = WIN if part is None else HALF
        groups = size // 8

        def ahead(g, ss):
            for s in ss:
                at = pl.ds(g * GROUP + s, 8, stride=PITCH)
                for c in range(2):
                    aheads[g % 2][c, 8 * s:8 * s + 8, :] = next_block(spec[c, at, :])

        def behind(g, ss):
            for s in ss:
                at = pl.ds(g * GROUP + s, 8, stride=PITCH)
                for c in range(2):
                    here = pl.ds(8 * s, 8)
                    cols[c, at, :] = nears[g % 2][c, here, :] + pltpu.roll(fars[g % 2][c, here, :], 1, 1)

        energy = jnp.zeros((8, lanes), jnp.float32)
        for h in range(2):
            values = []
            for t in range(WIN):
                at = pl.ds((t % HALF) * HALF + 8 * h, 8)
                values.append((z[buffer, upper + t // HALF, 0, at, :], z[buffer, upper + t // HALF, 1, at, :]))
            for real, imag in values:
                energy = energy + (real * real + imag * imag)
            if part == 0:
                values = [plus(values[t], values[t + HALF]) for t in range(HALF)]
            if part == 1:
                values = [rotated(minus(values[t], values[t + HALF]), *twiddle(t, WIN)) for t in range(HALF)]
            for k, value in enumerate(fft(values)):
                for c in range(2):
                    spec[c, pl.ds(k * PITCH + 8 * h, 8), :] = value[c]
            ahead(0, range(8 * h, 8 * h + 8))
        energy = jnp.broadcast_to(jnp.sum(energy, axis=0, keepdims=True), (8, lanes))
        energy = energy + next_block(energy) + EPS
        fourth = lax.rsqrt(energy * lax.rsqrt(energy)) / (WIN * WIN)
        kept = jnp.where(lane == lanes - 1, 0.0, fourth)
        for s in range(HALF):
            weights[0, 8 * s:8 * s + 8, :] = fourth * ramp(s)
            weights[1, 8 * s:8 * s + 8, :] = kept * ramp(s + HALF)

        for g in range(groups):
            if g + 1 < groups:
                ahead(g + 1, range(HALF))
            if g > 0:
                behind(g - 1, range(HALF))
            values = []
            for s in range(HALF):
                at = pl.ds(g * GROUP + s, 8, stride=PITCH)
                values.append((spec[0, at, :], spec[1, at, :]))
            for s in range(HALF):
                here = pl.ds(8 * s, 8)
                values.append((aheads[g % 2][0, here, :], aheads[g % 2][1, here, :]))
            shaped = []
            for real, imag in fft(values):
                gain = lax.rsqrt(lax.rsqrt(jnp.maximum(real * real + imag * imag, 1e-37)))
                shaped.append((real * gain, imag * gain))
            back = inverse_fft(shaped)
            for s in range(HALF):
                here = pl.ds(8 * s, 8)
                for c in range(2):
                    nears[g % 2][c, here, :] = back[s][c] * weights[0, here, :]
                    fars[g % 2][c, here, :] = back[s + HALF][c] * weights[1, here, :]

        for h in range(2):
            behind(groups - 1, range(8 * h, 8 * h + 8))
            values = []
            for k in range(size):
                at = pl.ds(k * PITCH + 8 * h, 8)
                values.append((cols[0, at, :], cols[1, at, :]))
            result = inverse_fft(values)
            if part == 1:
                result = [turned(value, *twiddle(t, WIN)) for t, value in enumerate(result)]
            for t in range(WIN):
                at = pl.ds((t % HALF) * HALF + 8 * h, 8)
                value = result[t % size]
                weight = -ramp(t) if part == 1 and t >= HALF else ramp(t)
                for c in range(2):
                    if part is None:
                        z[1 - buffer, upper + t // HALF, c, at, :] += value[c] * weight
                    else:
                        z[1 - buffer, upper + t // HALF, c, at, :] = value[c] * weight

    def middle(buffer):
        for part in range(2):
            @pl.when(lax.rem(me, 2) == part)
            def _(part=part):
                window_row(buffer, 3 * (1 - part), part)

    def give(step, which):
        buffer = (step + 1) % 2
        slot = pair_slot if which == 0 else own_slot
        return pltpu.make_async_remote_copy(
            src_ref=z.at[buffer, slot, :, pl.ds(0, AREA)], dst_ref=got.at[step, which],
            send_sem=give_sem.at[step, which], recv_sem=take_sem.at[step, which],
            device_id={"rows": me + side}, device_id_type=mesh,
        )

    def outer(buffer, q):
        upper = 1 + lax.rem(me, 2) * (q - 1) + (1 - lax.rem(me, 2)) * (2 - q)
        start = me + lax.rem(me, 2) * (q - 1) - (1 - lax.rem(me, 2)) * q
        far_slot = 2 - side * (q - 1)

        @pl.when(inside(start))
        def _():
            clear(1 - buffer, far_slot)
            window_row(buffer, upper, None)

        @pl.when(start + 1 == n)
        def _():
            clear(1 - buffer, far_slot)

    def settle(step, which):
        slot = own_slot if which == 0 else pair_slot
        buffer = (step + 1) % 2
        give(step, which).wait_recv()
        give(step, 1 - which).wait_send()
        for c in range(2):
            z[buffer, slot, c, 0:AREA] = z[buffer, slot, c, 0:AREA] + got[step, which, c]

    def tell(d):
        other = lax.rem(me + d, n)
        return pltpu.make_async_remote_copy(
            src_ref=mine.at[pl.ds(0, ITERS)], dst_ref=heard.at[n - d, pl.ds(0, ITERS)], send_sem=tell_sem.at[d], recv_sem=hear_sem.at[n - d],
            device_id={"rows": other}, device_id_type=mesh,
        )

    mine[...] = jnp.zeros_like(mine)
    enter(own, own_slot)
    advance(0)

    @pl.loop(0, 9)
    def _(i):
        def at(*turns):
            return functools.reduce(jnp.logical_or, [i == turn for turn in turns])

        def choose(table):
            return sum(jnp.where(i == turn, value, 0) for turn, value in table.items())

        central = at(0, 3, 7)
        step = choose({3: 1, 4: 1, 6: 1, 7: 2, 8: 2})
        q = choose({1: 1, 2: 2, 4: 1, 5: 3, 6: 2, 8: 1})
        buffer = lax.rem(step, 2)

        @pl.when(i == 2)
        def _():
            arrive(2 - 2 * side, -3 * side)

        @pl.when(i <= 2)
        def _():
            k = choose({0: -1, 1: 1, 2: 2})
            arrive(2 - side * (k - 1), -side * k)

        @pl.when(central)
        def _():
            middle(buffer)

        @pl.when(jnp.logical_not(central))
        def _():
            outer(buffer, q)

        @pl.when(i == 0)
        def _():
            give(0, 0).start()
            advance(1)

        @pl.when(i == 1)
        def _():
            give(0, 1).start()
            profile(0, 0)

        @pl.when(i == 2)
        def _():
            settle(0, 0)
            settle(0, 1)

        @pl.when(i == 3)
        def _():
            give(1, 0).start()

        @pl.when(i == 4)
        def _():
            give(1, 1).start()
            advance(2)
            profile(1, 1)

        @pl.when(i == 6)
        def _():
            settle(1, 0)
            settle(1, 1)
            profile(0, 2)
            advance(3, last=True)

            @pl.loop(1, n)
            def _(d):
                tell(d).start()

        @pl.when(i == 7)
        def _():
            give(2, 0).start()

    last = ITERS - 1
    give(last, 0).wait_recv()
    for c in range(2):
        for th in range(2):
            stack = [[None] * 2 for _ in range(8)]
            for h in range(2):
                pieces = []
                for t in range(8):
                    at = (8 * th + t) * HALF + 8 * h
                    pieces.append(z[ITERS % 2, own_slot, c, at:at + 8, :] + got[last, 0, c, at:at + 8, :])
                for b, block in enumerate(swap_blocks(pieces)):
                    stack[b][h] = block
            flat = jnp.concatenate([stack[b][h] for b in range(8) for h in range(2)], axis=0).T
            for k in range(16):
                out_ref[c, 8 * th:8 * th + 8, 128 * k:128 * k + 128] = flat[8 * k:8 * k + 8]
    give(last, 0).wait_send()

    for index, (d, slot) in enumerate(outgoing):
        @pl.when(inside(me + d))
        def _(d=d, slot=slot, index=index):
            phase_copy(d, slot, index).wait_send()

    def listen(d, total):
        tell(d).wait_send()
        pltpu.make_async_remote_copy(
            src_ref=mine.at[pl.ds(0, ITERS)], dst_ref=heard.at[d, pl.ds(0, ITERS)], send_sem=tell_sem.at[d], recv_sem=hear_sem.at[d],
            device_id={"rows": lax.rem(me + d, n)}, device_id_type=mesh,
        ).wait_recv()
        return total + heard[d, 0:ITERS, :]

    sums = lax.fori_loop(1, n, listen, mine[0:ITERS, :])
    tiles = prof_ref.shape[1]
    per_tile = lanes // tiles
    rows = lax.broadcasted_iota(jnp.int32, (lanes, tiles), 0)
    low = lax.broadcasted_iota(jnp.int32, (lanes, tiles), 1) * per_tile
    member = jnp.where(jnp.logical_and(rows >= low, rows < low + per_tile), 1.0, 0.0)
    energy = jnp.dot(sums, member, precision=lax.Precision.HIGHEST, preferred_element_type=jnp.float32)
    prof_ref[...] = energy / (HALF * n * 128.0)


def per_device(n, phase):
    slab, width = phase.shape
    assert ITERS == 3 and slab == HALF and n % 2 == 0 and width == 128 * HALF
    lanes = width // HALF
    vmem = pltpu.VMEM
    f32 = jnp.float32
    field, energy = pl.pallas_call(
        functools.partial(kernel, n, lanes),
        out_shape=(vmem((2, slab, width), f32), vmem((ITERS, width // 128), f32)),
        in_specs=[pl.BlockSpec(memory_space=pl.ANY)],
        out_specs=(pl.BlockSpec(memory_space=vmem), pl.BlockSpec(memory_space=vmem)),
        scratch_shapes=[
            vmem((slab, width), f32),
            pltpu.SemaphoreType.DMA,
            vmem((AREA, lanes), f32),
            vmem((SLABS, AREA, lanes), f32),
            vmem((2, SLABS, 2, AREA + SKEW, lanes), f32),
            vmem((2, WIN * PITCH + SKEW, lanes), f32),
            vmem((2, WIN * PITCH + SKEW, lanes), f32),
            *[vmem((2, 8 * HALF, lanes), f32) for _ in range(7)],
            vmem((8, lanes), f32),
            vmem((n, 8, lanes), f32),
            vmem((ITERS, 2, 2, AREA, lanes), f32),
            pltpu.SemaphoreType.DMA((4,)),
            pltpu.SemaphoreType.DMA((SLABS,)),
            pltpu.SemaphoreType.DMA((ITERS, 2)),
            pltpu.SemaphoreType.DMA((ITERS, 2)),
            pltpu.SemaphoreType.DMA((n,)),
            pltpu.SemaphoreType.DMA((n,)),
            pltpu.SemaphoreType.REGULAR((max(n.bit_length(), 1),)),
        ],
        compiler_params=pltpu.CompilerParams(collective_id=0, has_side_effects=True),
    )(phase)
    return pl.pallas_call(
        deliver,
        out_shape=(
            jax.ShapeDtypeStruct((2, slab, width), f32),
            jax.ShapeDtypeStruct((ITERS, width // 128), f32),
        ),
        in_specs=[pl.BlockSpec(memory_space=vmem)] * 2,
        out_specs=(pl.BlockSpec(memory_space=pl.ANY), pl.BlockSpec(memory_space=pl.ANY)),
        scratch_shapes=[pltpu.SemaphoreType.DMA((5,))],
    )(pltpu.with_memory_space_constraint(field, vmem), pltpu.with_memory_space_constraint(energy, vmem))


def deliver(field, energy, field_out, energy_out, sem):
    copies = [pltpu.make_async_copy(energy, energy_out, sem.at[0])]
    for c in range(2):
        for h in range(2):
            at = pl.ds(8 * h, 8)
            copies.append(pltpu.make_async_copy(field.at[c, at], field_out.at[c, at], sem.at[1 + 2 * c + h]))
    for copy in copies:
        copy.start()
    for copy in copies:
        copy.wait()


def solution(mesh):
    return jax.shard_map(
        functools.partial(per_device, mesh.shape["rows"]),
        mesh=mesh,
        in_specs=(P(("groups", "rows"), None),),
        out_specs=(P(None, ("groups", "rows"), None), P("groups", None)),
        check_vma=False,
    )
```

```python
import functools
import math

import jax
import jax.numpy as jnp
from jax import lax
from jax.experimental import pallas as pl
from jax.experimental.pallas import tpu as pltpu
from jax.sharding import PartitionSpec as P

ITERS = 3
HALF = 16
WIN = 32
EPS = 1e-06
SLABS = ITERS + 2
PITCH = HALF + 1
GROUP = 8 * PITCH
AREA = HALF * HALF
SKEW = 8


def rotated(value, cosine, sine):
    real, imag = value
    if sine == 0.0:
        return value
    if cosine == 0.0:
        return (imag, -real) if sine > 0 else (-imag, real)
    if abs(cosine - sine) < 1e-12:
        return ((real + imag) * cosine, (imag - real) * cosine)
    if abs(cosine + sine) < 1e-12:
        return ((real - imag) * cosine, (imag + real) * cosine)
    return (real * cosine + imag * sine, imag * cosine - real * sine)


def twiddle(power, size):
    power = power % size
    exact = {0: (1.0, 0.0), size // 4: (0.0, 1.0), size // 2: (-1.0, 0.0), 3 * size // 4: (0.0, -1.0)}
    if power in exact:
        return exact[power]
    angle = 2.0 * math.pi * power / size
    return math.cos(angle), math.sin(angle)


def plus(a, b):
    return (a[0] + b[0], a[1] + b[1])


def minus(a, b):
    return (a[0] - b[0], a[1] - b[1])


def fft(values):
    size = len(values)
    if size == 1:
        return values
    if size == 2:
        return [plus(values[0], values[1]), minus(values[0], values[1])]
    even = fft(values[0::2])
    first = fft(values[1::4])
    third = fft(values[3::4])
    quarter = size // 4
    result = [None] * size
    for k in range(quarter):
        p = rotated(first[k], *twiddle(k, size))
        q = rotated(third[k], *twiddle(3 * k, size))
        total = plus(p, q)
        gap = minus(p, q)
        result[k] = plus(even[k], total)
        result[k + 2 * quarter] = minus(even[k], total)
        base = even[k + quarter]
        result[k + quarter] = (base[0] + gap[1], base[1] - gap[0])
        result[k + 3 * quarter] = (base[0] - gap[1], base[1] + gap[0])
    return result


def inverse_fft(values):
    swapped = fft([(imag, real) for real, imag in values])
    return [(real, imag) for imag, real in swapped]


def ramp(offset):
    return 1.0 - abs(offset - (WIN - 1) / 2) / HALF


SIN = [0.999999995726543, -0.1666665798726027, 0.008333051039470773, -0.00019809078301890923, 2.6052402754334837e-06]
COS = [0.9999999533642212, -0.4999990525190427, 0.041663583530066516, -0.001385370173749607, 2.315398040033116e-05]


def polynomial(coefficients, x):
    total = coefficients[-1]
    for c in coefficients[-2::-1]:
        total = total * x + c
    return total


def cos_sin(x):
    u = x * 0.5
    u2 = u * u
    s = u * polynomial(SIN, u2)
    c = polynomial(COS, u2)
    return 1.0 - 2.0 * s * s, 2.0 * s * c


def turned(value, cosine, sine):
    real, imag = value
    imag, real = rotated((imag, real), cosine, sine)
    return real, imag


def swap_blocks(pieces):
    lane = lax.broadcasted_iota(jnp.int32, pieces[0].shape, 1)

    def pick(values):
        for bit in (1, 2, 4):
            chosen = (lane & bit) != 0
            values = [jnp.where(chosen, values[i ^ bit], values[i]) for i in range(8)]
        return values

    moved = pick(pieces)
    moved = [moved[0]] + [jnp.take_along_axis(moved[r], lane ^ r, axis=1) for r in range(1, 8)]
    return pick(moved)


def kernel(n, lanes, x_hbm, out_ref, prof_ref, x_ref, x_sem, own, ph, z, spec, cols, ahead_a, ahead_b, near_a, near_b,
           far_a, far_b, weights, mine, heard, got, send_sem, recv_sem, give_sem, take_sem, tell_sem, hear_sem, known_sem):
    me = lax.axis_index("rows")
    side = 1 - 2 * lax.rem(me, 2)
    even = side == 1
    mesh = pl.DeviceIdType.MESH

    def inside(index):
        return jnp.logical_and(index >= 0, index < n)

    barrier = pltpu.get_barrier_semaphore()
    close = [side, -side, 2 * side, -2 * side, -3 * side]
    for d in close:
        @pl.when(inside(me + d))
        def _(d=d):
            pl.semaphore_signal(barrier, inc=1, device_id={"rows": me + d}, device_id_type=mesh)

    fetch = pltpu.make_async_copy(x_hbm, x_ref, x_sem)
    fetch.start()

    lane = lax.broadcasted_iota(jnp.int32, (8, lanes), 1)
    sub = lax.broadcasted_iota(jnp.int32, (8, lanes), 0)

    def next_block(x):
        return jnp.where(lane == lanes - 1, 0.0, pltpu.roll(x, lanes - 1, 1))

    own_slot = 2 + side
    pair_slot = 2 + 2 * side

    fetch.wait()
    for th in range(2):
        rows = x_ref[8 * th:8 * th + 8, :]
        stack = jnp.concatenate([rows[:, 128 * c:128 * c + 128] for c in range(16)], axis=0).T
        for h in range(2):
            blocks = swap_blocks([stack[16 * b + 8 * h:16 * b + 8 * h + 8] for b in range(8)])
            for t in range(8):
                at = (8 * th + t) * HALF + 8 * h
                own[at:at + 8, :] = blocks[t]

    def enter(source, slot):
        @pl.loop(0, 2)
        def _(q):
            for i in range(16):
                at = pl.ds(pl.multiple_of(q * 128, 128) + 8 * i, 8)
                c, s = cos_sin(source[at, :])
                z[0, slot, 0, at, :] = c
                z[0, slot, 1, at, :] = s

    def clear(buffer, slot):
        for c in range(2):
            z[buffer, slot, c, 0:AREA] = jnp.zeros((AREA, lanes), jnp.float32)

    count = 0
    for d in close:
        count = count + inside(me + d).astype(jnp.int32)
    pl.semaphore_wait(barrier, count)

    def phase_copy(d, slot, index):
        return pltpu.make_async_remote_copy(
            src_ref=own, dst_ref=ph.at[slot], send_sem=send_sem.at[index], recv_sem=recv_sem.at[slot],
            device_id={"rows": me + d}, device_id_type=mesh,
        )

    outgoing = [(side, 2 - 2 * side), (-side, 2), (2 * side, 2 - side), (-3 * side, 2 + 2 * side)]
    for index, (d, slot) in enumerate(outgoing):
        @pl.when(inside(me + d))
        def _(d=d, slot=slot, index=index):
            phase_copy(d, slot, index).start()

    reach = 2
    rounds = []
    while reach < n - 1:
        rounds.append(reach)
        reach *= 2

    def announce(i):
        for d in (-rounds[i], rounds[i]):
            @pl.when(inside(me + d))
            def _(d=d):
                pl.semaphore_signal(known_sem.at[i], inc=1, device_id={"rows": me + d}, device_id_type=mesh)

    def confirm(i):
        total = inside(me - rounds[i]).astype(jnp.int32) + inside(me + rounds[i]).astype(jnp.int32)
        pl.semaphore_wait(known_sem.at[i], total)

    def advance(i, last=False):
        if i > 0 and i <= len(rounds):
            confirm(i - 1)
        if i < len(rounds):
            announce(i)
        if last:
            for j in range(i + 1, len(rounds) + 1):
                advance(j)

    def arrive(slot, away):
        source = me + away
        valid = inside(source)

        @pl.when(valid)
        def _():
            pltpu.make_async_remote_copy(
                src_ref=own, dst_ref=ph.at[slot], send_sem=send_sem.at[0], recv_sem=recv_sem.at[slot],
                device_id={"rows": source}, device_id_type=mesh,
            ).wait_recv()
            enter(ph.at[slot], slot)

        @pl.when(jnp.logical_not(valid))
        def _():
            clear(0, slot)

    def profile(buffer, step):
        def row(slot, t):
            halves = []
            for c in range(2):
                base = t * HALF
                low = z[buffer, slot, c, pl.ds(base, 8), :]
                high = z[buffer, slot, c, pl.ds(base + 8, 8), :]
                low_next = z[buffer, slot, c, pl.ds(base + 1, 8), :]
                high_next = jnp.where(sub == 7, next_block(low)[0:1], z[buffer, slot, c, pl.ds(base + 9, 8), :])
                halves.append(((low, low_next), (high, high_next)))
            real, imag = halves
            return [(real[h][0], imag[h][0], real[h][1], imag[h][1]) for h in range(2)]

        def add(upper, lower, total):
            for u, v in zip(upper, lower):
                pr, pi = u[0] - v[2], u[1] - v[3]
                qr, qi = u[2] - v[0], u[3] - v[1]
                loop = pi * qr - pr * qi
                total = total + loop * loop
            return total

        def four(q, total):
            rows = [row(own_slot, 5 * q + t) for t in range(6)]
            for t in range(5):
                total = add(rows[t], rows[t + 1], total)
            return total

        total = lax.fori_loop(0, 3, four, jnp.zeros((8, lanes), jnp.float32))
        total = add(row(own_slot, HALF - 1), row(own_slot + 1, 0), total)
        mine[step:step + 1, :] = jnp.sum(total, axis=0, keepdims=True)

    aheads, nears, fars = (ahead_a, ahead_b), (near_a, near_b), (far_a, far_b)

    def window_row(buffer, upper, part):
        size = WIN if part is None else HALF
        groups = size // 8

        def ahead(g, ss):
            for s in ss:
                at = pl.ds(g * GROUP + s, 8, stride=PITCH)
                for c in range(2):
                    aheads[g % 2][c, 8 * s:8 * s + 8, :] = next_block(spec[c, at, :])

        def behind(g, ss):
            for s in ss:
                at = pl.ds(g * GROUP + s, 8, stride=PITCH)
                for c in range(2):
                    here = pl.ds(8 * s, 8)
                    cols[c, at, :] = nears[g % 2][c, here, :] + pltpu.roll(fars[g % 2][c, here, :], 1, 1)

        energy = jnp.zeros((8, lanes), jnp.float32)
        for h in range(2):
            values = []
            for t in range(WIN):
                at = pl.ds((t % HALF) * HALF + 8 * h, 8)
                values.append((z[buffer, upper + t // HALF, 0, at, :], z[buffer, upper + t // HALF, 1, at, :]))
            for real, imag in values:
                energy = energy + (real * real + imag * imag)
            if part == 0:
                values = [plus(values[t], values[t + HALF]) for t in range(HALF)]
            if part == 1:
                values = [rotated(minus(values[t], values[t + HALF]), *twiddle(t, WIN)) for t in range(HALF)]
            for k, value in enumerate(fft(values)):
                for c in range(2):
                    spec[c, pl.ds(k * PITCH + 8 * h, 8), :] = value[c]
            ahead(0, range(8 * h, 8 * h + 8))
        energy = jnp.broadcast_to(jnp.sum(energy, axis=0, keepdims=True), (8, lanes))
        energy = energy + next_block(energy) + EPS
        fourth = lax.rsqrt(energy * lax.rsqrt(energy)) / (WIN * WIN)
        kept = jnp.where(lane == lanes - 1, 0.0, fourth)
        for s in range(HALF):
            weights[0, 8 * s:8 * s + 8, :] = fourth * ramp(s)
            weights[1, 8 * s:8 * s + 8, :] = kept * ramp(s + HALF)

        for g in range(groups):
            if g + 1 < groups:
                ahead(g + 1, range(HALF))
            if g > 0:
                behind(g - 1, range(HALF))
            values = []
            for s in range(HALF):
                at = pl.ds(g * GROUP + s, 8, stride=PITCH)
                values.append((spec[0, at, :], spec[1, at, :]))
            for s in range(HALF):
                here = pl.ds(8 * s, 8)
                values.append((aheads[g % 2][0, here, :], aheads[g % 2][1, here, :]))
            shaped = []
            for real, imag in fft(values):
                gain = lax.rsqrt(lax.rsqrt(jnp.maximum(real * real + imag * imag, 1e-37)))
                shaped.append((real * gain, imag * gain))
            back = inverse_fft(shaped)
            for s in range(HALF):
                here = pl.ds(8 * s, 8)
                for c in range(2):
                    nears[g % 2][c, here, :] = back[s][c] * weights[0, here, :]
                    fars[g % 2][c, here, :] = back[s + HALF][c] * weights[1, here, :]

        for h in range(2):
            behind(groups - 1, range(8 * h, 8 * h + 8))
            values = []
            for k in range(size):
                at = pl.ds(k * PITCH + 8 * h, 8)
                values.append((cols[0, at, :], cols[1, at, :]))
            result = inverse_fft(values)
            if part == 1:
                result = [turned(value, *twiddle(t, WIN)) for t, value in enumerate(result)]
            for t in range(WIN):
                at = pl.ds((t % HALF) * HALF + 8 * h, 8)
                value = result[t % size]
                weight = -ramp(t) if part == 1 and t >= HALF else ramp(t)
                for c in range(2):
                    if part is None:
                        z[1 - buffer, upper + t // HALF, c, at, :] += value[c] * weight
                    else:
                        z[1 - buffer, upper + t // HALF, c, at, :] = value[c] * weight

    def middle(buffer):
        for part in range(2):
            @pl.when(lax.rem(me, 2) == part)
            def _(part=part):
                window_row(buffer, 3 * (1 - part), part)

    def give(step, which):
        buffer = (step + 1) % 2
        slot = pair_slot if which == 0 else own_slot
        return pltpu.make_async_remote_copy(
            src_ref=z.at[buffer, slot, :, pl.ds(0, AREA)], dst_ref=got.at[step, which],
            send_sem=give_sem.at[step, which], recv_sem=take_sem.at[step, which],
            device_id={"rows": me + side}, device_id_type=mesh,
        )

    def outer(buffer, q):
        upper = 1 + lax.rem(me, 2) * (q - 1) + (1 - lax.rem(me, 2)) * (2 - q)
        start = me + lax.rem(me, 2) * (q - 1) - (1 - lax.rem(me, 2)) * q
        far_slot = 2 - side * (q - 1)

        @pl.when(inside(start))
        def _():
            clear(1 - buffer, far_slot)
            window_row(buffer, upper, None)

        @pl.when(start + 1 == n)
        def _():
            clear(1 - buffer, far_slot)

    def settle(step, which):
        slot = own_slot if which == 0 else pair_slot
        buffer = (step + 1) % 2
        give(step, which).wait_recv()
        give(step, 1 - which).wait_send()
        for c in range(2):
            z[buffer, slot, c, 0:AREA] = z[buffer, slot, c, 0:AREA] + got[step, which, c]

    def tell(d):
        other = lax.rem(me + d, n)
        return pltpu.make_async_remote_copy(
            src_ref=mine.at[pl.ds(0, ITERS)], dst_ref=heard.at[n - d, pl.ds(0, ITERS)], send_sem=tell_sem.at[d], recv_sem=hear_sem.at[n - d],
            device_id={"rows": other}, device_id_type=mesh,
        )

    mine[...] = jnp.zeros_like(mine)
    enter(own, own_slot)
    advance(0)

    @pl.loop(0, 9)
    def _(i):
        def at(*turns):
            return functools.reduce(jnp.logical_or, [i == turn for turn in turns])

        def choose(table):
            return sum(jnp.where(i == turn, value, 0) for turn, value in table.items())

        central = at(0, 3, 7)
        step = choose({3: 1, 4: 1, 6: 1, 7: 2, 8: 2})
        q = choose({1: 1, 2: 2, 4: 1, 5: 3, 6: 2, 8: 1})
        buffer = lax.rem(step, 2)

        @pl.when(i == 2)
        def _():
            arrive(2 - 2 * side, -3 * side)

        @pl.when(i <= 2)
        def _():
            k = choose({0: -1, 1: 1, 2: 2})
            arrive(2 - side * (k - 1), -side * k)

        @pl.when(central)
        def _():
            middle(buffer)

        @pl.when(jnp.logical_not(central))
        def _():
            outer(buffer, q)

        @pl.when(i == 0)
        def _():
            give(0, 0).start()
            advance(1)

        @pl.when(i == 1)
        def _():
            give(0, 1).start()
            profile(0, 0)

        @pl.when(i == 2)
        def _():
            settle(0, 0)
            settle(0, 1)

        @pl.when(i == 3)
        def _():
            give(1, 0).start()

        @pl.when(i == 4)
        def _():
            give(1, 1).start()
            advance(2)
            profile(1, 1)

        @pl.when(i == 6)
        def _():
            settle(1, 0)
            settle(1, 1)
            profile(0, 2)
            advance(3, last=True)

            @pl.loop(1, n)
            def _(d):
                tell(d).start()

        @pl.when(i == 7)
        def _():
            give(2, 0).start()

    last = ITERS - 1
    give(last, 0).wait_recv()
    for c in range(2):
        for th in range(2):
            stack = [[None] * 2 for _ in range(8)]
            for h in range(2):
                pieces = []
                for t in range(8):
                    at = (8 * th + t) * HALF + 8 * h
                    pieces.append(z[ITERS % 2, own_slot, c, at:at + 8, :] + got[last, 0, c, at:at + 8, :])
                for b, block in enumerate(swap_blocks(pieces)):
                    stack[b][h] = block
            flat = jnp.concatenate([stack[b][h] for b in range(8) for h in range(2)], axis=0).T
            for k in range(16):
                out_ref[c, 8 * th:8 * th + 8, 128 * k:128 * k + 128] = flat[8 * k:8 * k + 8]
    give(last, 0).wait_send()

    for index, (d, slot) in enumerate(outgoing):
        @pl.when(inside(me + d))
        def _(d=d, slot=slot, index=index):
            phase_copy(d, slot, index).wait_send()

    def listen(d, total):
        tell(d).wait_send()
        pltpu.make_async_remote_copy(
            src_ref=mine.at[pl.ds(0, ITERS)], dst_ref=heard.at[d, pl.ds(0, ITERS)], send_sem=tell_sem.at[d], recv_sem=hear_sem.at[d],
            device_id={"rows": lax.rem(me + d, n)}, device_id_type=mesh,
        ).wait_recv()
        return total + heard[d, 0:ITERS, :]

    sums = lax.fori_loop(1, n, listen, mine[0:ITERS, :])
    tiles = prof_ref.shape[1]
    per_tile = lanes // tiles
    rows = lax.broadcasted_iota(jnp.int32, (lanes, tiles), 0)
    low = lax.broadcasted_iota(jnp.int32, (lanes, tiles), 1) * per_tile
    member = jnp.where(jnp.logical_and(rows >= low, rows < low + per_tile), 1.0, 0.0)
    energy = jnp.dot(sums, member, precision=lax.Precision.HIGHEST, preferred_element_type=jnp.float32)
    prof_ref[...] = energy / (HALF * n * 128.0)


def per_device(n, phase):
    slab, width = phase.shape
    assert ITERS == 3 and slab == HALF and n % 2 == 0 and width == 128 * HALF
    lanes = width // HALF
    vmem = pltpu.VMEM
    f32 = jnp.float32
    field, energy = pl.pallas_call(
        functools.partial(kernel, n, lanes),
        out_shape=(vmem((2, slab, width), f32), vmem((ITERS, width // 128), f32)),
        in_specs=[pl.BlockSpec(memory_space=pl.ANY)],
        out_specs=(pl.BlockSpec(memory_space=vmem), pl.BlockSpec(memory_space=vmem)),
        scratch_shapes=[
            vmem((slab, width), f32),
            pltpu.SemaphoreType.DMA,
            vmem((AREA, lanes), f32),
            vmem((SLABS, AREA, lanes), f32),
            vmem((2, SLABS, 2, AREA + SKEW, lanes), f32),
            vmem((2, WIN * PITCH + SKEW, lanes), f32),
            vmem((2, WIN * PITCH + SKEW, lanes), f32),
            *[vmem((2, 8 * HALF, lanes), f32) for _ in range(7)],
            vmem((8, lanes), f32),
            vmem((n, 8, lanes), f32),
            vmem((ITERS, 2, 2, AREA, lanes), f32),
            pltpu.SemaphoreType.DMA((4,)),
            pltpu.SemaphoreType.DMA((SLABS,)),
            pltpu.SemaphoreType.DMA((ITERS, 2)),
            pltpu.SemaphoreType.DMA((ITERS, 2)),
            pltpu.SemaphoreType.DMA((n,)),
            pltpu.SemaphoreType.DMA((n,)),
            pltpu.SemaphoreType.REGULAR((max(n.bit_length(), 1),)),
        ],
        compiler_params=pltpu.CompilerParams(collective_id=0, has_side_effects=True),
    )(phase)
    return pl.pallas_call(
        deliver,
        out_shape=(
            jax.ShapeDtypeStruct((2, slab, width), f32),
            jax.ShapeDtypeStruct((ITERS, width // 128), f32),
        ),
        in_specs=[pl.BlockSpec(memory_space=vmem)] * 2,
        out_specs=(pl.BlockSpec(memory_space=pl.ANY), pl.BlockSpec(memory_space=pl.ANY)),
        scratch_shapes=[pltpu.SemaphoreType.DMA((5,))],
    )(pltpu.with_memory_space_constraint(field, vmem), pltpu.with_memory_space_constraint(energy, vmem))


def deliver(field, energy, field_out, energy_out, sem):
    copies = [pltpu.make_async_copy(energy, energy_out, sem.at[0])]
    for c in range(2):
        for h in range(2):
            at = pl.ds(8 * h, 8)
            copies.append(pltpu.make_async_copy(field.at[c, at], field_out.at[c, at], sem.at[1 + 2 * c + h]))
    for copy in copies:
        copy.start()
    for copy in copies:
        copy.wait()


def solution(mesh):
    return jax.shard_map(
        functools.partial(per_device, mesh.shape["rows"]),
        mesh=mesh,
        in_specs=(P(("groups", "rows"), None),),
        out_specs=(P(None, ("groups", "rows"), None), P("groups", None)),
        check_vma=False,
    )
```
